512 devices in a mesh: lat: 32 (over z_lo, y), lon: 16 (over z_hi, x, core).
Axes of the slice: x: 4, y: 4, z: 16 (z_hi: 2, z_lo: 8; z = z_hi * 8 + z_lo), core: 2. Of those that a mesh axis runs over, the one named last changes fastest.
Arguments:
- grid_field: float32 [384, 256, 2048], P(None, 'lat', 'lon'), may hold values from -6 to 6
- disco_dlat: int32 [256, 16], P('lat'), may hold values from -2 to 2
- disco_dlon: int32 [256, 16], P('lat'), may hold values from -2 to 2
- disco_basis: int32 [256, 16], P('lat'), may hold values from 0 to 3
- disco_quad: float32 [256, 16], P('lat'), may hold values from 0.05 to 0.5
- disco_weight: bfloat16 [4, 384, 384], replicated, may hold values from -0.3125 to 0.3125
- norm_gain: float32 [384], replicated, may hold values from 0.1 to 1.9
- spectral_filter: float32 [384, 256], replicated, may hold values from -6 to 6
- mix_weight: bfloat16 [384, 384], replicated, may hold values from -0.3125 to 0.3125
Outputs:
- updated: float32 [384, 256, 2048], P(None, 'lat', 'lon')
The draws below stay inside these ranges and needn't reach their ends.
All inputs are finite; a program needn't handle non-finite values.
Results may differ from the reference program's by a relative error of at most 0.0044.
Values may be sent and summed in bfloat16 or wider, within the bound.
No kernel may reach another device: no remote copies, remote signals or barrier semaphores. Data moves between devices by JAX's collectives and lax.ppermute only.
A program may use at most 64 MiB of HBM per device.

```python
import math
import jax
import jax.numpy as jnp
from jax import lax

C = 384
HALO = 2
KSUP = 16
NBASIS = 4
NLAT = 256
NLON = 2048
MM = 256
LL = 256


def plant(result, stream_key, least, top_value):
    place = [jax.random.randint(jax.random.fold_in(stream_key, axis), (), 0, length) for axis, length in enumerate(result.shape)]
    widest = result.shape.index(max(result.shape))
    beside = place[:widest] + [(place[widest] + 1) % result.shape[widest]] + place[widest + 1:]
    return result.at[tuple(place)].set(least).at[tuple(beside)].set(top_value)


def block_levels(stream_key, extent, split, least, largest):
    def one(position, blocks):
        steps = jax.random.uniform(jax.random.fold_in(jax.random.fold_in(stream_key, 6), position), (blocks,), jnp.float32, least / len(split), largest / len(split))
        return jnp.repeat(jnp.exp(steps), extent[position] // blocks).reshape((-1,) + (1,) * (len(extent) - position - 1))

    gain = one(*split[0])
    for cut in split[1:]:
        gain = gain * one(*cut)
    return gain


def centred(stream_key, dims, deviation, reach, shards=(), kind=jnp.bfloat16):
    array = deviation * jax.random.normal(stream_key, dims, jnp.float32)
    if shards:
        array = array * block_levels(stream_key, dims, shards, -0.22, 0.18)
    return jnp.clip(array, -reach, reach).astype(kind)


def setup_inputs(seed: int = 0) -> dict:
    key_of = jax.random.split(jax.random.key(seed), 10)
    return {
        "grid_field": centred(key_of[0], (C, NLAT, NLON), 1.0, 6.0, ((1, 32), (2, 16)), jnp.float32),
        "disco_dlat": plant(jax.random.randint(key_of[1], (NLAT, KSUP), -HALO, HALO + 1), jax.random.fold_in(key_of[1], 1), -HALO, HALO).astype(jnp.int32),
        "disco_dlon": plant(jax.random.randint(key_of[2], (NLAT, KSUP), -HALO, HALO + 1), jax.random.fold_in(key_of[2], 1), -HALO, HALO).astype(jnp.int32),
        "disco_basis": plant(jax.random.randint(key_of[3], (NLAT, KSUP), 0, NBASIS), jax.random.fold_in(key_of[3], 1), 0, NBASIS - 1).astype(jnp.int32),
        "disco_quad": jnp.clip(jnp.exp(math.log(0.5) - 2.3025851 * jax.random.uniform(key_of[4], (NLAT, KSUP), jnp.float32) ** block_levels(key_of[4], (NLAT, KSUP), ((0, 32),), -0.2, 0.2)), 0.05, 0.5),
        "disco_weight": centred(key_of[5], (NBASIS, C, C), C ** -0.5, 0.3125),
        "norm_gain": jnp.clip(1.0 + 0.18 * jax.random.normal(key_of[6], (C,), jnp.float32), 0.1, 1.9),
        "spectral_filter": centred(key_of[7], (C, LL), 1.0, 6.0, (), jnp.float32),
        "mix_weight": centred(key_of[8], (C, C), C ** -0.5, 0.3125),
    }


def legendre_table(first_order, local_orders, all_orders, degrees, nlat):
    lat_pos = jnp.arange(nlat, dtype=jnp.float32)
    colatitude = math.pi * (lat_pos + 0.5) / nlat
    cosine = jnp.cos(colatitude)
    sine = jnp.sin(colatitude)
    counters = jnp.arange(1, all_orders, dtype=jnp.float32)
    cumulative = jnp.concatenate([jnp.zeros((1,), jnp.float32), jnp.cumsum(jnp.log((2.0 * counters - 1.0) / (2.0 * counters)))])
    log_product = lax.dynamic_slice_in_dim(cumulative, first_order, local_orders)
    orders = first_order + jnp.arange(local_orders, dtype=jnp.int32)
    order_real = orders.astype(jnp.float32)[:, None]
    log_seed = 0.5 * (jnp.log((2.0 * order_real + 1.0) / (4.0 * math.pi)) + log_product[:, None]) + order_real * jnp.log(sine)[None, :]
    rescale = jnp.clip(-log_seed, 0.0, 80.0)
    seed_value = jnp.exp(log_seed + rescale)
    undo = jnp.exp(-rescale)

    def advance(state_pair, degree):
        previous, before_last = state_pair
        degree_real = degree.astype(jnp.float32)
        factor_a = jnp.sqrt(jnp.maximum(4.0 * degree_real ** 2 - 1.0, 1.0) / jnp.maximum(degree_real ** 2 - order_real ** 2, 1.0))
        factor_b = jnp.sqrt(jnp.maximum((degree_real - 1.0) ** 2 - order_real ** 2, 0.0) / jnp.maximum(4.0 * (degree_real - 1.0) ** 2 - 1.0, 1.0))
        recurred = factor_a * (cosine[None, :] * previous - factor_b * before_last)
        current = jnp.where(degree == orders[:, None], seed_value, jnp.where(degree > orders[:, None], recurred, 0.0))
        return ((current, previous), current * undo)
    empty = jnp.zeros((local_orders, nlat), jnp.float32)
    final_pair, table = lax.scan(advance, (empty, empty), jnp.arange(degrees, dtype=jnp.int32), unroll=8)
    return table

def disco_rows(padded, disco_dlat, disco_dlon, disco_basis, disco_quad, disco_weight, width):
    basis_count = disco_weight.shape[0]
    channels = padded.shape[0]
    zero_index = jnp.zeros((), jnp.int32)

    def one_row(inputs):
        row_index, lat_offsets, lon_offsets, basis_row, quad_row = inputs
        sources = (row_index + HALO + lat_offsets).astype(jnp.int32)
        begins = (HALO + lon_offsets).astype(jnp.int32)

        def take(source, begin):
            return lax.dynamic_slice(padded, (zero_index, source, begin), (channels, 1, width))[:, 0, :]
        support = jax.vmap(take)(sources, begins)
        selector = (basis_row[:, None] == jnp.arange(basis_count, dtype=jnp.int32)[None, :]).astype(jnp.float32) * quad_row[:, None]
        aggregate = jnp.einsum('kb,kcj->bcj', selector, support, precision=lax.Precision.HIGHEST).astype(jnp.bfloat16)
        return lax.dot_general(disco_weight, aggregate, (((0, 1), (0, 1)), ((), ())), preferred_element_type=jnp.float32)
    row_count = disco_dlat.shape[0]
    stacked = lax.map(one_row, (jnp.arange(row_count, dtype=jnp.int32), disco_dlat, disco_dlon, disco_basis, disco_quad))
    return jnp.transpose(stacked, (1, 0, 2))

def reference(grid_field, disco_dlat, disco_dlon, disco_basis, disco_quad, disco_weight, norm_gain, spectral_filter, mix_weight):
    padded = jnp.pad(grid_field, ((0, 0), (HALO, HALO), (0, 0)))
    padded = jnp.concatenate([padded[:, :, NLON - HALO:], padded, padded[:, :, :HALO]], axis=2)
    after_conv = grid_field + disco_rows(padded, disco_dlat, disco_dlon, disco_basis, disco_quad, disco_weight, NLON)
    mean_square = lax.optimization_barrier(jnp.mean(after_conv * after_conv, axis=0, keepdims=True))
    normed = after_conv * lax.rsqrt(mean_square + 1e-06) * norm_gain[:, None, None]
    spectrum = jnp.fft.rfft(normed, axis=2)[:, :, :MM] * (2.0 * math.pi / NLON)
    fourier = jnp.stack([jnp.real(spectrum), jnp.imag(spectrum)]).astype(jnp.float32)
    lat_pos = jnp.arange(NLAT, dtype=jnp.float32)
    quad_weight = math.pi / NLAT * jnp.sin(math.pi * (lat_pos + 0.5) / NLAT)
    weighted = jnp.transpose(fourier, (3, 0, 1, 2)) * quad_weight
    table = legendre_table(0, MM, MM, LL, NLAT)

    def per_order(inputs):
        portion, order_table = inputs
        spectra = jnp.einsum('rck,lk->rcl', portion, order_table, precision=lax.Precision.HIGHEST)
        filtered = spectra * spectral_filter[None]
        return jnp.einsum('rcl,lk->rck', filtered, order_table, precision=lax.Precision.HIGHEST)
    synthesis = lax.map(per_order, (weighted, jnp.transpose(table, (1, 0, 2))))
    complex_part = lax.complex(synthesis[:, 0], synthesis[:, 1])
    complex_part = jnp.transpose(complex_part, (1, 2, 0))
    complex_part = jnp.pad(complex_part, ((0, 0), (0, 0), (0, NLON // 2 + 1 - MM)))
    wave_field = (jnp.fft.irfft(complex_part, n=NLON, axis=2) * NLON).astype(jnp.float32)
    activated = jax.nn.gelu(wave_field, approximate=True).astype(jnp.bfloat16)
    mixed = jnp.dot(jnp.transpose(mix_weight), activated.reshape(C, NLAT * NLON), preferred_element_type=jnp.float32)
    return after_conv + mixed.reshape(C, NLAT, NLON)
```

```python
import math

import jax
import jax.numpy as jnp
import numpy as np
from jax import lax
from jax.experimental import pallas as pl
from jax.experimental.pallas import tpu as pltpu
from jax.sharding import Mesh
from jax.sharding import PartitionSpec as P

C = 384
NLAT = 256
NLON = 2048
MM = 256
LL = 256
KSUP = 16
NBASIS = 4
TL = 8
JL = 128
CB = 12
ORD = 16
LAT = ("zl", "y")
LON = ("zh", "x", "core")
CHAN = ("y", "x", "core")
RING = ("zh", "zl")
F32 = jnp.float32
BF16 = jnp.bfloat16


def call(kernel, name, out_shape, in_specs=None, scratch=(), grid=None, out_specs=None):
    kwargs = {}
    if grid is not None:
        kwargs["grid"] = grid
    if in_specs is not None:
        kwargs["in_specs"] = in_specs
    if out_specs is not None:
        kwargs["out_specs"] = out_specs
    return pl.pallas_call(
        kernel,
        out_shape=out_shape,
        scratch_shapes=list(scratch),
        name=name,
        compiler_params=pltpu.CompilerParams(vmem_limit_bytes=60 * 1024 * 1024),
        **kwargs,
    )


def shape(dims, kind=BF16):
    return jax.ShapeDtypeStruct(dims, kind)


def dot(a, b, dims=((1,), (0,))):
    return lax.dot_general(a, b, (dims, ((), ())), preferred_element_type=F32)


def two_parts(value):
    high = value.astype(BF16)
    return high, (value - high.astype(F32)).astype(BF16)


def split_constant(table):
    high = table.astype(np.float32).astype(jnp.bfloat16)
    low = (table - high.astype(np.float64)).astype(np.float32).astype(jnp.bfloat16)
    return high, low


def longitude_tables():
    order = np.arange(MM)
    lon = np.arange(NLON // 2)
    phase = (order[:, None] * lon[None, :] % NLON) * (2.0 * math.pi / NLON)
    cosine, sine = np.cos(phase), -np.sin(phase)
    both = np.stack([cosine, sine]).reshape(2, MM // ORD, ORD, NLON // 2)
    both = both.transpose(1, 0, 2, 3).reshape(2 * MM, NLON // 2)
    weight = np.where(order == 0, 1.0, 2.0).reshape(MM // ORD, 1, ORD)
    weight = np.broadcast_to(weight, (MM // ORD, 2, ORD)).reshape(2 * MM, 1)
    return split_constant(both * (2.0 * math.pi / NLON)), split_constant(both * weight)


def lane_order():
    y, c, t = np.meshgrid(np.arange(4), np.arange(CB), np.arange(TL), indexing="ij")
    src = (y * CB + c) * TL + t
    dst = ((c // 4 * 4 + y) * TL + t) * 4 + c % 4
    out = np.zeros((4 * CB * TL, 4 * CB * TL), np.float32)
    out[src.ravel(), dst.ravel()] = 1.0
    return out.astype(jnp.bfloat16)


def latitude_rows():
    lane = np.arange(NLAT)
    lat = lane % 8 * 32 + lane // 8
    colat = math.pi * (lat + 0.5) / NLAT
    rows = np.zeros((8, NLAT), np.float32)
    rows[0] = np.cos(colat)
    rows[1] = np.log(np.sin(colat))
    rows[2] = math.pi / NLAT * np.sin(colat)
    return rows


def order_terms():
    order = np.arange(MM, dtype=np.float64)
    steps = np.zeros(MM)
    steps[1:] = np.cumsum(np.log((2.0 * order[1:] - 1.0) / (2.0 * order[1:])))
    term = 0.5 * (np.log((2.0 * order + 1.0) / (4.0 * math.pi)) + steps)
    return np.repeat(term[:, None], 128, axis=1).astype(np.float32)


def degree_terms():
    degree = np.arange(LL, dtype=np.float64)
    return np.stack(
        [
            np.sqrt(np.maximum(4.0 * degree**2 - 1.0, 1.0)),
            1.0 / np.sqrt(np.maximum(4.0 * (degree - 1.0) ** 2 - 1.0, 1.0)),
        ]
    ).astype(np.float32)


def rows_kernel(x_ref, first_ref, last_ref):
    for u in range(2):
        first_ref[pl.ds(u * C, C), :] = x_ref[pl.ds(u, C, stride=TL), :].astype(BF16)
        last_ref[pl.ds(u * C, C), :] = x_ref[pl.ds(TL - 2 + u, C, stride=TL), :].astype(BF16)


def edges_kernel(x_ref, up_ref, down_ref, head_ref, tail_ref):
    row = lax.broadcasted_iota(jnp.int32, (64, JL), 0)
    lane = lax.broadcasted_iota(jnp.int32, (64, JL), 1)
    total = jnp.zeros((64, C), F32)
    for r in range(12):
        if r < 2:
            cells = up_ref[pl.ds(r * C, C), :]
        elif r < 10:
            cells = x_ref[pl.ds(r - 2, C, stride=TL), :].astype(BF16)
        else:
            cells = down_ref[pl.ds((r - 10) * C, C), :]
        pick = ((row - 2 * r == lane) & (lane < 2)) | ((row - 32 - 2 * r == lane - (JL - 2)) & (lane >= JL - 2))
        total = total + dot(pick.astype(F32).astype(BF16), cells, ((1,), (1,)))
    head_ref[...] = total[:32].astype(BF16)
    tail_ref[...] = total[32:].astype(BF16)


def weights_kernel(w_ref, mix_ref, wt_ref, mixt_ref):
    wt_ref[...] = w_ref[...].T
    mixt_ref[...] = mix_ref[...].T


def legendre_kernel(
    place_ref, degree_ref, term_ref, lat_ref, fwd_hi, fwd_lo, inv_hi, inv_lo, left_ref, right_ref
):
    first = place_ref[0] * ORD
    order = (first + lax.broadcasted_iota(jnp.int32, (ORD, 128), 0)).astype(F32)
    squared = order * order
    term = term_ref[pl.ds(pl.multiple_of(first, ORD), ORD), :]
    cosines, seeds, undos = [], [], []
    for h in range(2):
        lanes = pl.ds(128 * h, 128)
        log_seed = term + order * lat_ref[pl.ds(1, 1), lanes]
        rescale = jnp.clip(-log_seed, 0.0, 80.0)
        cosines.append(jnp.broadcast_to(lat_ref[pl.ds(0, 1), lanes], (ORD, 128)))
        seeds.append(jnp.exp(log_seed + rescale))
        undos.append(jnp.exp(-rescale))
    refs = (left_ref, right_ref)

    def advance(degree, state):
        real = degree.astype(F32)
        below = real - 1.0
        a = degree_ref[0, degree] * lax.rsqrt(jnp.maximum(real * real - squared, 1.0))
        b = degree_ref[1, degree] * jnp.sqrt(jnp.maximum(below * below - squared, 0.0))
        found = []
        for h in range(2):
            last, before = state[2 * h], state[2 * h + 1]
            recurred = a * (cosines[h] * last - b * before)
            current = jnp.where(
                order == real, seeds[h], jnp.where(order < real, recurred, 0.0)
            )
            refs[h][pl.ds(pl.multiple_of(degree * ORD, ORD), ORD), :] = current * undos[h]
            found += [current, last]
        return tuple(found)

    empty = order * 0.0 * seeds[0]
    lax.fori_loop(0, LL, advance, (empty,) * 4, unroll=4)
    quad = lat_ref[pl.ds(2, 1), :]
    for m in range(ORD):
        table = jnp.concatenate(
            [left_ref[pl.ds(m, LL, stride=ORD), :], right_ref[pl.ds(m, LL, stride=ORD), :]], axis=1
        )
        fwd_hi[m], fwd_lo[m] = two_parts(table * quad)
        inv_hi[m], inv_lo[m] = two_parts(table.T)


def conv_kernel(
    dlat_ref,
    dlon_ref,
    basis_ref,
    quad_ref,
    x_ref,
    up_ref,
    down_ref,
    west_ref,
    east_ref,
    wt_ref,
    gain_ref,
    after_ref,
    normed_ref,
    shifted_ref,
    sums_ref,
    scaled_ref,
):
    row = lax.broadcasted_iota(jnp.int32, (64, JL), 0)
    lane = lax.broadcasted_iota(jnp.int32, (64, JL), 1)
    lanes = lax.broadcasted_iota(jnp.int32, (C, JL), 1)
    edges = jnp.concatenate([west_ref[...], east_ref[...]], axis=0).astype(F32).T.astype(BF16)
    for r in range(12):
        if r < 2:
            cells = up_ref[pl.ds(r * C, C), :].astype(F32)
        elif r < 10:
            cells = x_ref[pl.ds(r - 2, C, stride=TL), :]
        else:
            cells = down_ref[pl.ds((r - 10) * C, C), :].astype(F32)
        west = (row - 2 * r == lane - (JL - 2)) & (lane >= JL - 2)
        east = (row - 32 - 2 * r == lane) & (lane < 2)
        edge = dot(edges, (west | east).astype(F32).astype(BF16))
        for s in range(5):
            by = s - 2
            if by > 0:
                moved = pltpu.roll(jnp.where(lanes < by, edge, cells), JL - by, 1)
            elif by < 0:
                moved = pltpu.roll(jnp.where(lanes >= JL + by, edge, cells), -by, 1)
            else:
                moved = cells
            shifted_ref[s * 12 + r] = moved

    def one_row(t, carry):
        sums_ref[...] = jnp.zeros((NBASIS, C, JL), F32)
        for k in range(KSUP):
            b = basis_ref[t, k]
            place = (dlon_ref[t, k] + 2) * 12 + dlat_ref[t, k] + 2 + t
            sums_ref[b] = sums_ref[b] + quad_ref[t, k] * shifted_ref[place]
        aggregate = sums_ref[...].astype(BF16).reshape(NBASIS * C, JL)
        rows = pl.ds(t, C, stride=TL)
        after = x_ref[rows, :] + dot(wt_ref[...], aggregate)
        after_ref[rows, :] = after
        inverse = lax.rsqrt(jnp.sum(after * after, axis=0, keepdims=True) * (1.0 / C) + 1e-6)
        scaled_ref[rows, :] = after * inverse * gain_ref[...]
        return carry

    lax.fori_loop(0, TL, one_row, 0)
    normed_ref[...] = scaled_ref[...].astype(BF16)


def fourier_kernel(recv_ref, hi_ref, lo_ref, lane_ref, out_ref):
    circles = jnp.concatenate(
        [
            jnp.concatenate([recv_ref[8 * y + s] for s in range(8)], axis=1)
            for y in range(4)
        ],
        axis=0,
    )
    dims = ((1,), (1,))
    found = dot(hi_ref[...], circles, dims) + dot(lo_ref[...], circles, dims)
    out_ref[...] = dot(found.astype(BF16), lane_ref[...]).astype(BF16)


def spectral_kernel(
    recv_ref, fwd_hi, fwd_lo, inv_hi, inv_lo, filter_ref, out_ref, in_ref, rows_ref, back_ref
):
    m = pl.program_id(0)
    sign = (1 - 2 * (m % 2)).astype(F32)

    @pl.when(m == 0)
    def _():
        for j in range(3):
            in_ref[j] = recv_ref[:, 128 * j : 128 * (j + 1)].astype(F32)

    lane = lax.broadcasted_iota(jnp.int32, (8, 128), 1)
    parts = []
    for r in range(2):
        for j in range(3):
            near = in_ref[j, pl.ds(r * ORD + m, 8, stride=32), :]
            far = in_ref[j, pl.ds(256 + r * ORD + m, 8, stride=32), :]
            parts.append(near + sign * far)
    for yt in range(32):
        tile = None
        for n in range(6):
            moved = pltpu.roll(parts[n], (4 * n - 4 * yt) % 128, 1)
            tile = moved if tile is None else jnp.where(lane >= 4 * n, moved, tile)
        rows_ref[pl.ds(8 * yt, 8), :] = tile
    fields = rows_ref[...].astype(BF16)
    spectra = dot(fwd_hi[0], fields) + dot(fwd_lo[0], fields)
    filtered = (spectra * filter_ref[...]).astype(BF16)
    synthesis = dot(inv_hi[0], filtered) + dot(inv_lo[0], filtered)
    rows_ref[...] = synthesis
    found = [None] * 6
    for yt in range(32):
        tile = rows_ref[pl.ds(8 * yt, 8), :]
        for n in range(6):
            moved = pltpu.roll(tile, (4 * yt - 4 * n) % 128, 1)
            found[n] = moved if yt == 0 else jnp.where(lane >= 4 * yt, moved, found[n])
    for r in range(2):
        for j in range(3):
            value = found[3 * r + j]
            back_ref[j, pl.ds(r * ORD + m, 8, stride=32), :] = value
            back_ref[j, pl.ds(256 + r * ORD + m, 8, stride=32), :] = sign * value

    @pl.when(m == ORD - 1)
    def _():
        for j in range(3):
            out_ref[:, 128 * j : 128 * (j + 1)] = back_ref[j].astype(BF16)


def inverse_kernel(recv_ref, hi_ref, lo_ref, lane_ref, out_ref):
    turned = dot(lane_ref[...], recv_ref[...], ((1,), (1,))).astype(BF16)
    for s in range(8):
        lons = pl.ds(128 * s, 128)
        wave = dot(turned, hi_ref[:, lons]) + dot(turned, lo_ref[:, lons])
        act = jax.nn.gelu(wave, approximate=True).astype(BF16)
        for y in range(4):
            out_ref[8 * y + s] = act[96 * y : 96 * (y + 1)]


def mix_kernel(act_ref, after_ref, mixt_ref, out_ref, wide_ref):
    wide_ref[...] = act_ref[...].astype(F32)
    for t in range(TL):
        rows = pl.ds(t, C, stride=TL)
        mixed = dot(mixt_ref[...], wide_ref[rows, :].astype(BF16))
        out_ref[rows, :] = after_ref[rows, :] + mixed


def exchanged(blocks, axes):
    return lax.all_to_all(blocks, axes, split_axis=0, concat_axis=0, tiled=True)


def per_device(
    grid_field,
    disco_dlat,
    disco_dlon,
    disco_basis,
    disco_quad,
    disco_weight,
    norm_gain,
    spectral_filter,
    mix_weight,
):
    (fwd_hi, fwd_lo), (inv_hi, inv_lo) = longitude_tables()
    lanes = lane_order()
    smem = pl.BlockSpec(memory_space=pltpu.SMEM)
    vmem = pl.BlockSpec(memory_space=pltpu.VMEM)
    x = grid_field.reshape(C * TL, JL)

    lat_count = lax.axis_size(LAT)
    lon_count = lax.axis_size(LON)
    first, last = call(rows_kernel, "rows", (shape((2 * C, JL)), shape((2 * C, JL))))(x)
    up = lax.ppermute(last, LAT, [(i, i + 1) for i in range(lat_count - 1)])
    down = lax.ppermute(first, LAT, [(i + 1, i) for i in range(lat_count - 1)])
    head, tail = call(edges_kernel, "edges", (shape((32, C)), shape((32, C))))(x, up, down)
    west = lax.ppermute(tail, LON, [(i, (i + 1) % lon_count) for i in range(lon_count)])
    east = lax.ppermute(head, LON, [((i + 1) % lon_count, i) for i in range(lon_count)])

    wt, mixt = call(weights_kernel, "weights", (shape((C, NBASIS * C)), shape((C, C))))(
        disco_weight.reshape(NBASIS * C, C), mix_weight
    )
    place = lax.axis_index(RING).astype(jnp.int32).reshape(1)
    tables = call(
        legendre_kernel,
        "legendre",
        (shape((ORD, LL, NLAT)),) * 2 + (shape((ORD, NLAT, LL)),) * 2,
        in_specs=[smem, smem, vmem, vmem],
        scratch=(pltpu.VMEM((LL * ORD, 128), F32), pltpu.VMEM((LL * ORD, 128), F32)),
    )(place, degree_terms(), order_terms(), latitude_rows())
    own = lax.dynamic_slice_in_dim(spectral_filter, lax.axis_index(CHAN) * CB, CB, 0)
    own = jnp.concatenate([own, own, jnp.zeros((128 - 2 * CB, LL), F32)], axis=0).T
    gain = jnp.broadcast_to(norm_gain[:, None], (C, JL))

    after, normed = call(
        conv_kernel,
        "conv",
        (shape((C * TL, JL), F32), shape((C * TL, JL))),
        in_specs=[smem] * 4 + [vmem] * 7,
        scratch=(
            pltpu.VMEM((60, C, JL), F32),
            pltpu.VMEM((NBASIS, C, JL), F32),
            pltpu.VMEM((C * TL, JL), F32),
        ),
    )(disco_dlat, disco_dlon, disco_basis, disco_quad, x, up, down, west, east, wt, gain)

    portion = exchanged(normed.reshape(32, CB * TL, JL), CHAN)
    fourier = call(fourier_kernel, "fourier", shape((2 * MM, C)))(portion, fwd_hi, fwd_lo, lanes)
    gathered = exchanged(fourier.reshape(16, 2 * ORD, C), RING)
    whole = pl.BlockSpec((2 * MM, C), lambda m: (0, 0))
    table = pl.BlockSpec((1, LL, NLAT), lambda m: (m, 0, 0))
    synthesis = call(
        spectral_kernel,
        "spectral",
        shape((2 * MM, C)),
        grid=(ORD,),
        in_specs=[whole] + [table] * 4 + [pl.BlockSpec((LL, 128), lambda m: (0, 0))],
        out_specs=whole,
        scratch=(
            pltpu.VMEM((3, 2 * MM, 128), F32),
            pltpu.VMEM((NLAT, 128), F32),
            pltpu.VMEM((3, 2 * MM, 128), F32),
        ),
    )(gathered.reshape(2 * MM, C), *tables, own)
    returned = exchanged(synthesis.reshape(16, 2 * ORD, C), RING)
    activated = call(inverse_kernel, "inverse", shape((32, CB * TL, JL)))(
        returned.reshape(2 * MM, C), inv_hi, inv_lo, lanes
    )
    mixed = exchanged(activated, CHAN)
    out = call(
        mix_kernel, "mix", shape((C * TL, JL), F32), scratch=(pltpu.VMEM((C * TL, JL), F32),)
    )(mixed.reshape(C * TL, JL), after, mixt)
    return out.reshape(C, TL, JL)


def solution(mesh):
    torus = Mesh(mesh.devices.reshape(8, 4, 2, 4, 2), ("zl", "y", "zh", "x", "core"))
    placed = (P(None, LAT, LON),) + (P(LAT, None),) * 4 + (P(),) * 4
    return jax.shard_map(
        per_device, mesh=torus, in_specs=placed, out_specs=P(None, LAT, LON), check_vma=False
    )
```

```python
import math

import jax
import jax.numpy as jnp
import numpy as np
from jax import lax
from jax.experimental import pallas as pl
from jax.experimental.pallas import tpu as pltpu
from jax.sharding import Mesh
from jax.sharding import PartitionSpec as P

C = 384
NLAT = 256
NLON = 2048
MM = 256
LL = 256
KSUP = 16
NBASIS = 4
TL = 8
JL = 128
CB = 12
ORD = 16
STEP = 4
LAT = ("zl", "y")
LON = ("zh", "x", "core")
CHAN = ("y", "x", "core")
RING = ("zh", "zl")
F32 = jnp.float32
BF16 = jnp.bfloat16


def call(kernel, name, mib, out_shape, in_specs=None, scratch=(), grid=None, out_specs=None):
    kwargs = {}
    if grid is not None:
        kwargs["grid"] = grid
    if in_specs is not None:
        kwargs["in_specs"] = in_specs
    if out_specs is not None:
        kwargs["out_specs"] = out_specs
    return pl.pallas_call(
        kernel,
        out_shape=out_shape,
        scratch_shapes=list(scratch),
        name=name,
        compiler_params=pltpu.CompilerParams(vmem_limit_bytes=mib * 1024 * 1024),
        **kwargs,
    )


def shape(dims, kind=BF16):
    return jax.ShapeDtypeStruct(dims, kind)


def dot(a, b, dims=((1,), (0,))):
    return lax.dot_general(a, b, (dims, ((), ())), preferred_element_type=F32)


def two_parts(value):
    high = value.astype(BF16)
    return high, (value - high.astype(F32)).astype(BF16)


def split_constant(table):
    high = table.astype(np.float32).astype(jnp.bfloat16)
    low = (table - high.astype(np.float64)).astype(np.float32).astype(jnp.bfloat16)
    return high, low


def longitude_tables():
    order = np.arange(MM)
    lon = np.arange(NLON // 2)
    phase = (order[:, None] * lon[None, :] % NLON) * (2.0 * math.pi / NLON)
    cosine, sine = np.cos(phase), -np.sin(phase)
    both = np.stack([cosine, sine]).reshape(2, MM // ORD, ORD, NLON // 2)
    both = both.transpose(1, 0, 2, 3).reshape(2 * MM, NLON // 2)
    weight = np.where(order == 0, 1.0, 2.0).reshape(MM // ORD, 1, ORD)
    weight = np.broadcast_to(weight, (MM // ORD, 2, ORD)).reshape(2 * MM, 1)
    return split_constant(both * (2.0 * math.pi / NLON)), split_constant(both * weight)


def lane_order():
    y, c, t = np.meshgrid(np.arange(4), np.arange(CB), np.arange(TL), indexing="ij")
    src = (y * CB + c) * TL + t
    dst = ((c // 4 * 4 + y) * TL + t) * 4 + c % 4
    out = np.zeros((4 * CB * TL, 4 * CB * TL), np.float32)
    out[src.ravel(), dst.ravel()] = 1.0
    return out.astype(jnp.bfloat16)


def latitude_rows():
    lane = np.arange(NLAT)
    lat = lane % 8 * 32 + lane // 8
    colat = math.pi * (lat + 0.5) / NLAT
    rows = np.zeros((8, NLAT), np.float32)
    rows[0] = np.cos(colat)
    rows[1] = np.log(np.sin(colat))
    rows[2] = math.pi / NLAT * np.sin(colat)
    return rows


def order_terms():
    order = np.arange(MM, dtype=np.float64)
    steps = np.zeros(MM)
    steps[1:] = np.cumsum(np.log((2.0 * order[1:] - 1.0) / (2.0 * order[1:])))
    term = 0.5 * (np.log((2.0 * order + 1.0) / (4.0 * math.pi)) + steps)
    return np.repeat(term[:, None], 128, axis=1).astype(np.float32)


def degree_terms():
    degree = np.arange(LL, dtype=np.float64)
    return np.stack(
        [
            np.sqrt(np.maximum(4.0 * degree**2 - 1.0, 1.0)),
            1.0 / np.sqrt(np.maximum(4.0 * (degree - 1.0) ** 2 - 1.0, 1.0)),
        ]
    ).astype(np.float32)


def rows_kernel(x_ref, first_ref, last_ref):
    for u in range(2):
        first_ref[pl.ds(u * C, C), :] = x_ref[pl.ds(u, C, stride=TL), :].astype(BF16)
        last_ref[pl.ds(u * C, C), :] = x_ref[pl.ds(TL - 2 + u, C, stride=TL), :].astype(BF16)


def edges_kernel(core_ref, x_ref, up_ref, down_ref, far_ref, near_ref):
    row = lax.broadcasted_iota(jnp.int32, (64, JL), 0)
    lane = lax.broadcasted_iota(jnp.int32, (64, JL), 1)
    total = jnp.zeros((64, C), F32)
    for r in range(12):
        if r < 2:
            cells = up_ref[pl.ds(r * C, C), :]
        elif r < 10:
            cells = x_ref[pl.ds(r - 2, C, stride=TL), :].astype(BF16)
        else:
            cells = down_ref[pl.ds((r - 10) * C, C), :]
        head = (row - 2 * r == lane) & (lane < 2)
        tail = (row - 32 - 2 * r == lane - (JL - 2)) & (lane >= JL - 2)
        total = total + dot((head | tail).astype(F32).astype(BF16), cells, ((1,), (1,)))
    odd = core_ref[0] == 1
    far_ref[...] = jnp.where(odd, total[32:], total[:32]).astype(BF16)
    near_ref[...] = jnp.where(odd, total[:32], total[32:]).astype(BF16)


def weights_kernel(w_ref, mix_ref, norm_ref, wt_ref, mixt_ref, gain_ref):
    gain_ref[...] = jnp.broadcast_to(norm_ref[...], (JL, C)).T
    wt_ref[...] = w_ref[...].T
    mixt_ref[...] = mix_ref[...].T


def legendre_kernel(
    place_ref, degree_ref, term_ref, lat_ref, table_ref, left_ref, right_ref
):
    first = place_ref[0] * ORD
    order = (first + lax.broadcasted_iota(jnp.int32, (ORD, 128), 0)).astype(F32)
    squared = order * order
    term = term_ref[pl.ds(pl.multiple_of(first, ORD), ORD), :]
    cosines, seeds, undos = [], [], []
    for h in range(2):
        lanes = pl.ds(128 * h, 128)
        log_seed = term + order * lat_ref[pl.ds(1, 1), lanes]
        rescale = jnp.clip(-log_seed, 0.0, 80.0)
        cosines.append(jnp.broadcast_to(lat_ref[pl.ds(0, 1), lanes], (ORD, 128)))
        seeds.append(jnp.exp(log_seed + rescale))
        undos.append(jnp.exp(-rescale))
    refs = (left_ref, right_ref)

    def advance(degree, state):
        real = degree.astype(F32)
        below = real - 1.0
        a = degree_ref[0, degree] * lax.rsqrt(jnp.maximum(real * real - squared, 1.0))
        b = degree_ref[1, degree] * jnp.sqrt(jnp.maximum(below * below - squared, 0.0))
        found = []
        for h in range(2):
            last, before = state[2 * h], state[2 * h + 1]
            recurred = a * (cosines[h] * last - b * before)
            current = jnp.where(
                order == real, seeds[h], jnp.where(order < real, recurred, 0.0)
            )
            refs[h][pl.ds(pl.multiple_of(degree * ORD, ORD), ORD), :] = current * undos[h]
            found += [current, last]
        return tuple(found)

    empty = order * 0.0 * seeds[0]
    lax.fori_loop(0, LL, advance, (empty,) * 4, unroll=4)
    quad = lat_ref[pl.ds(2, 1), :]
    for m in range(ORD):
        table = jnp.concatenate(
            [left_ref[pl.ds(m, LL, stride=ORD), :], right_ref[pl.ds(m, LL, stride=ORD), :]], axis=1
        )
        table_ref[0, m], table_ref[1, m] = two_parts(table * quad)
        table_ref[2, m], table_ref[3, m] = two_parts(table.T)


def conv_kernel(
    dlat_ref,
    dlon_ref,
    basis_ref,
    quad_ref,
    x_ref,
    up_ref,
    down_ref,
    wt_ref,
    after_ref,
    shifted_ref,
    sums_ref,
):
    lanes = lax.broadcasted_iota(jnp.int32, (C, JL), 1)
    for r in range(12):
        if r < 2:
            cells = up_ref[pl.ds(r * C, C), :].astype(F32)
        elif r < 10:
            cells = x_ref[pl.ds(r - 2, C, stride=TL), :]
        else:
            cells = down_ref[pl.ds((r - 10) * C, C), :].astype(F32)
        for s in range(5):
            by = s - 2
            if by > 0:
                moved = jnp.where(lanes < JL - by, pltpu.roll(cells, JL - by, 1), 0.0)
            elif by < 0:
                moved = jnp.where(lanes >= -by, pltpu.roll(cells, -by, 1), 0.0)
            else:
                moved = cells
            shifted_ref[s * 12 + r] = moved

    def one_row(t, carry):
        sums_ref[...] = jnp.zeros((NBASIS, C, JL), F32)
        for k in range(KSUP):
            b = basis_ref[t, k]
            place = (dlon_ref[t, k] + 2) * 12 + dlat_ref[t, k] + 2 + t
            sums_ref[b] = sums_ref[b] + quad_ref[t, k] * shifted_ref[place]
        aggregate = sums_ref[...].astype(BF16).reshape(NBASIS * C, JL)
        rows = pl.ds(t, C, stride=TL)
        after_ref[rows, :] = x_ref[rows, :] + dot(wt_ref[...], aggregate)
        return carry

    lax.fori_loop(0, TL, one_row, 0)


def seam_kernel(
    core_ref,
    dlat_ref,
    dlon_ref,
    basis_ref,
    quad_ref,
    inner_ref,
    far_ref,
    near_ref,
    wt_ref,
    gain_ref,
    after_ref,
    normed_ref,
    scaled_ref,
):
    even = core_ref[0] == 0
    far = far_ref[...].astype(F32)
    near = near_ref[...].astype(F32)
    west = jnp.where(even, far, near)
    east = jnp.where(even, near, far)
    edges = jnp.concatenate([west, east], axis=0).T.astype(BF16)
    row = lax.broadcasted_iota(jnp.int32, (64, 128), 0)
    lane = lax.broadcasted_iota(jnp.int32, (8, 128), 1)
    own = (lane >> 2) & 7
    col = lane & 3
    gather = jnp.zeros((64, 128), F32)
    for k in range(KSUP):
        dlat = jnp.zeros((8, 128), jnp.int32)
        dlon = dlat
        basis = dlat
        quad = jnp.zeros((8, 128), F32)
        for t in range(TL):
            here = own == t
            dlat = jnp.where(here, dlat_ref[t, k], dlat)
            dlon = jnp.where(here, dlon_ref[t, k], dlon)
            basis = jnp.where(here, basis_ref[t, k], basis)
            quad = jnp.where(here, quad_ref[t, k], quad)
        start = 2 * (own + 2 + dlat)
        cell = col + dlon
        source = jnp.where(
            col < 2,
            jnp.where(cell >= 2, 32 + start + cell - 2, -1),
            jnp.where(cell < 2, start + cell, -1),
        )
        source = jnp.where(basis == lane >> 5, source, -1)
        gather = gather + jnp.where(
            row == jnp.concatenate([source] * 8, axis=0), jnp.concatenate([quad] * 8, axis=0), 0.0
        )
    high, low = two_parts(gather)
    sums = dot(edges, high) + dot(edges, low)
    aggregate = jnp.concatenate(
        [sums.astype(BF16)]
        + [pltpu.roll(sums, 128 - 32 * b, 1).astype(BF16) for b in range(1, NBASIS)],
        axis=0,
    )
    seam = dot(wt_ref[...], aggregate)
    lanes = lax.broadcasted_iota(jnp.int32, (C, JL), 1)
    outer = (lanes < 2) | (lanes >= JL - 2)
    for t in range(TL):
        rows = pl.ds(t, C, stride=TL)
        moved = pltpu.roll(seam, (JL - 2 - 4 * t) % JL, 1)
        after = inner_ref[rows, :] + jnp.where(outer, moved, 0.0)
        after_ref[rows, :] = after
        inverse = lax.rsqrt(jnp.sum(after * after, axis=0, keepdims=True) * (1.0 / C) + 1e-6)
        scaled_ref[rows, :] = after * inverse * gain_ref[...]
    normed_ref[...] = scaled_ref[...].astype(BF16)


def fourier_kernel(recv_ref, hi_ref, lo_ref, lane_ref, out_ref):
    circles = jnp.concatenate(
        [
            jnp.concatenate([recv_ref[8 * y + s] for s in range(8)], axis=1)
            for y in range(4)
        ],
        axis=0,
    )
    dims = ((1,), (1,))
    found = dot(hi_ref[...], circles, dims) + dot(lo_ref[...], circles, dims)
    out_ref[...] = dot(found.astype(BF16), lane_ref[...]).astype(BF16)


def spectral_kernel(
    recv_ref, table_ref, filter_ref, out_ref, in_ref, rows_ref, back_ref
):
    first = pl.program_id(0) * STEP

    @pl.when(first == 0)
    def _():
        for j in range(3):
            in_ref[j] = recv_ref[:, 128 * j : 128 * (j + 1)].astype(F32)

    lane = lax.broadcasted_iota(jnp.int32, (8, 128), 1)
    for i in range(STEP):
        parts = []
        for r in range(2):
            for j in range(3):
                near = in_ref[j, pl.ds(r * ORD + first + i, 8, stride=32), :]
                far = in_ref[j, pl.ds(256 + r * ORD + first + i, 8, stride=32), :]
                parts.append(near - far if i % 2 else near + far)
        for yt in range(32):
            tile = None
            for n in range(6):
                moved = pltpu.roll(parts[n], (4 * n - 4 * yt) % 128, 1)
                tile = moved if tile is None else jnp.where(lane >= 4 * n, moved, tile)
            rows_ref[i, pl.ds(8 * yt, 8), :] = tile
    filtered = []
    for i in range(STEP):
        fields = rows_ref[i].astype(BF16)
        spectra = dot(table_ref[0, i], fields) + dot(table_ref[1, i], fields)
        filtered.append((spectra * filter_ref[...]).astype(BF16))
    for i in range(STEP):
        rows_ref[i] = dot(table_ref[2, i], filtered[i]) + dot(table_ref[3, i], filtered[i])
    for i in range(STEP):
        found = [None] * 6
        for yt in range(32):
            tile = rows_ref[i, pl.ds(8 * yt, 8), :]
            for n in range(6):
                moved = pltpu.roll(tile, (4 * yt - 4 * n) % 128, 1)
                found[n] = moved if yt == 0 else jnp.where(lane >= 4 * yt, moved, found[n])
        for r in range(2):
            for j in range(3):
                value = found[3 * r + j]
                back_ref[j, pl.ds(r * ORD + first + i, 8, stride=32), :] = value
                back_ref[j, pl.ds(256 + r * ORD + first + i, 8, stride=32), :] = (
                    -value if i % 2 else value
                )

    @pl.when(first == ORD - STEP)
    def _():
        for j in range(3):
            out_ref[:, 128 * j : 128 * (j + 1)] = back_ref[j].astype(BF16)


def inverse_kernel(recv_ref, hi_ref, lo_ref, lane_ref, out_ref):
    turned = dot(lane_ref[...], recv_ref[...], ((1,), (1,))).astype(BF16)
    for s in range(8):
        lons = pl.ds(128 * s, 128)
        wave = dot(turned, hi_ref[:, lons]) + dot(turned, lo_ref[:, lons])
        act = jax.nn.gelu(wave, approximate=True).astype(BF16)
        for y in range(4):
            out_ref[8 * y + s] = act[96 * y : 96 * (y + 1)]


def mix_kernel(act_ref, after_ref, mixt_ref, out_ref, wide_ref):
    wide_ref[...] = act_ref[...].astype(F32)
    for t in range(TL):
        rows = pl.ds(t, C, stride=TL)
        mixed = dot(mixt_ref[...], wide_ref[rows, :].astype(BF16))
        out_ref[rows, :] = after_ref[rows, :] + mixed


def exchanged(blocks, axes):
    return lax.all_to_all(blocks, axes, split_axis=0, concat_axis=0, tiled=True)


def pairs(count, first):
    ends = [(i, (i + 1) % count) for i in range(first, count, 2)]
    return ends + [(j, i) for i, j in ends]


def per_device(
    grid_field,
    disco_dlat,
    disco_dlon,
    disco_basis,
    disco_quad,
    disco_weight,
    norm_gain,
    spectral_filter,
    mix_weight,
):
    (fwd_hi, fwd_lo), (inv_hi, inv_lo) = longitude_tables()
    lanes = lane_order()
    smem = pl.BlockSpec(memory_space=pltpu.SMEM)
    vmem = pl.BlockSpec(memory_space=pltpu.VMEM)
    x = grid_field.reshape(C * TL, JL)

    lat_count = lax.axis_size(LAT)
    lon_count = lax.axis_size(LON)
    first, last = call(rows_kernel, "rows", 6, (shape((2 * C, JL)), shape((2 * C, JL))))(x)
    up = lax.ppermute(last, LAT, [(i, i + 1) for i in range(lat_count - 1)])
    down = lax.ppermute(first, LAT, [(i + 1, i) for i in range(lat_count - 1)])
    wt, mixt, gain = call(
        weights_kernel,
        "weights",
        10,
        (shape((C, NBASIS * C)), shape((C, C)), shape((C, JL), F32)),
    )(disco_weight.reshape(NBASIS * C, C), mix_weight, norm_gain.reshape(1, C))
    own = lax.dynamic_slice_in_dim(spectral_filter, lax.axis_index(CHAN) * CB, CB, 0)
    own = jnp.concatenate([own, own, jnp.zeros((128 - 2 * CB, LL), F32)], axis=0).T
    up, down, wt, mixt, gain, own = lax.optimization_barrier((up, down, wt, mixt, gain, own))
    core = lax.axis_index("core").astype(jnp.int32).reshape(1)
    far, near = call(
        edges_kernel, "edges", 6, (shape((32, C)), shape((32, C))), in_specs=[smem] + [vmem] * 3
    )(core, x, up, down)
    far = lax.ppermute(far, LON, pairs(lon_count, 1))
    near = lax.ppermute(near, LON, pairs(lon_count, 0))

    place = lax.axis_index(RING).astype(jnp.int32).reshape(1)
    tables = call(
        legendre_kernel,
        "legendre", 57,
        shape((4, ORD, LL, NLAT)),
        in_specs=[smem, smem, vmem, vmem],
        scratch=(pltpu.VMEM((LL * ORD, 128), F32), pltpu.VMEM((LL * ORD, 128), F32)),
    )(place, degree_terms(), order_terms(), latitude_rows())

    inner = call(
        conv_kernel,
        "conv", 24,
        shape((C * TL, JL), F32),
        in_specs=[smem] * 4 + [vmem] * 4,
        scratch=(pltpu.VMEM((60, C, JL), F32), pltpu.VMEM((NBASIS, C, JL), F32)),
    )(disco_dlat, disco_dlon, disco_basis, disco_quad, x, up, down, wt)
    after, normed = call(
        seam_kernel,
        "seam", 12,
        (shape((C * TL, JL), F32), shape((C * TL, JL))),
        in_specs=[smem] * 5 + [vmem] * 5,
        scratch=(pltpu.VMEM((C * TL, JL), F32),),
    )(core, disco_dlat, disco_dlon, disco_basis, disco_quad, inner, far, near, wt, gain)

    portion = exchanged(normed.reshape(32, CB * TL, JL), CHAN)
    fourier = call(fourier_kernel, "fourier", 16, shape((2 * MM, C)))(portion, fwd_hi, fwd_lo, lanes)
    gathered = exchanged(fourier.reshape(16, 2 * ORD, C), RING)
    whole = pl.BlockSpec((2 * MM, C), lambda m: (0, 0))
    table = pl.BlockSpec((4, STEP, LL, NLAT), lambda m: (0, m, 0, 0))
    synthesis = call(
        spectral_kernel,
        "spectral", 54,
        shape((2 * MM, C)),
        grid=(ORD // STEP,),
        in_specs=[whole, table, pl.BlockSpec((LL, 128), lambda m: (0, 0))],
        out_specs=whole,
        scratch=(
            pltpu.VMEM((3, 2 * MM, 128), F32),
            pltpu.VMEM((STEP, NLAT, 128), F32),
            pltpu.VMEM((3, 2 * MM, 128), F32),
        ),
    )(gathered.reshape(2 * MM, C), tables, own)
    returned = exchanged(synthesis.reshape(16, 2 * ORD, C), RING)
    activated = call(inverse_kernel, "inverse", 16, shape((32, CB * TL, JL)))(
        returned.reshape(2 * MM, C), inv_hi, inv_lo, lanes
    )
    mixed = exchanged(activated, CHAN)
    out = call(
        mix_kernel, "mix", 12, shape((C * TL, JL), F32), scratch=(pltpu.VMEM((C * TL, JL), F32),)
    )(mixed.reshape(C * TL, JL), after, mixt)
    return out.reshape(C, TL, JL)


def solution(mesh):
    torus = Mesh(mesh.devices.reshape(8, 4, 2, 4, 2), ("zl", "y", "zh", "x", "core"))
    placed = (P(None, LAT, LON),) + (P(LAT, None),) * 4 + (P(),) * 4
    return jax.shard_map(
        per_device, mesh=torus, in_specs=placed, out_specs=P(None, LAT, LON), check_vma=False
    )
```

```python
import math

import jax
import jax.numpy as jnp
import numpy as np
from jax import lax
from jax.experimental import pallas as pl
from jax.experimental.pallas import tpu as pltpu
from jax.sharding import Mesh
from jax.sharding import PartitionSpec as P

C = 384
NLAT = 256
NLON = 2048
MM = 256
LL = 256
KSUP = 16
NBASIS = 4
TL = 8
JL = 128
CB = 12
ORD = 16
STEP = 4
LAT = ("zl", "y")
LON = ("zh", "x", "core")
CHAN = ("y", "x", "core")
RING = ("zh", "zl")
F32 = jnp.float32
BF16 = jnp.bfloat16


def call(kernel, name, mib, out_shape, in_specs=None, scratch=(), grid=None, out_specs=None):
    kwargs = {}
    if grid is not None:
        kwargs["grid"] = grid
    if in_specs is not None:
        kwargs["in_specs"] = in_specs
    if out_specs is not None:
        kwargs["out_specs"] = out_specs
    return pl.pallas_call(
        kernel,
        out_shape=out_shape,
        scratch_shapes=list(scratch),
        name=name,
        compiler_params=pltpu.CompilerParams(vmem_limit_bytes=mib * 1024 * 1024),
        **kwargs,
    )


def shape(dims, kind=BF16):
    return jax.ShapeDtypeStruct(dims, kind)


def dot(a, b, dims=((1,), (0,))):
    return lax.dot_general(a, b, (dims, ((), ())), preferred_element_type=F32)


def two_parts(value):
    high = value.astype(BF16)
    return high, (value - high.astype(F32)).astype(BF16)


def split_constant(table):
    high = table.astype(np.float32).astype(jnp.bfloat16)
    low = (table - high.astype(np.float64)).astype(np.float32).astype(jnp.bfloat16)
    return high, low


def longitude_tables():
    order = np.arange(MM)
    lon = np.arange(NLON // 2)
    phase = (order[:, None] * lon[None, :] % NLON) * (2.0 * math.pi / NLON)
    cosine, sine = np.cos(phase), -np.sin(phase)
    both = np.stack([cosine, sine]).reshape(2, MM // ORD, ORD, NLON // 2)
    both = both.transpose(1, 0, 2, 3).reshape(2 * MM, NLON // 2)
    weight = np.where(order == 0, 1.0, 2.0).reshape(MM // ORD, 1, ORD)
    weight = np.broadcast_to(weight, (MM // ORD, 2, ORD)).reshape(2 * MM, 1)
    return split_constant(both * (2.0 * math.pi / NLON)), split_constant(both * weight)


def lane_order():
    y, c, t = np.meshgrid(np.arange(4), np.arange(CB), np.arange(TL), indexing="ij")
    src = (y * CB + c) * TL + t
    dst = ((c // 4 * 4 + y) * TL + t) * 4 + c % 4
    out = np.zeros((4 * CB * TL, 4 * CB * TL), np.float32)
    out[src.ravel(), dst.ravel()] = 1.0
    return out.astype(jnp.bfloat16)


def latitude_rows():
    lane = np.arange(NLAT)
    lat = lane % 8 * 32 + lane // 8
    colat = math.pi * (lat + 0.5) / NLAT
    rows = np.zeros((8, NLAT), np.float32)
    rows[0] = np.cos(colat)
    rows[1] = np.log(np.sin(colat))
    rows[2] = math.pi / NLAT * np.sin(colat)
    return rows


def order_terms():
    order = np.arange(MM, dtype=np.float64)
    steps = np.zeros(MM)
    steps[1:] = np.cumsum(np.log((2.0 * order[1:] - 1.0) / (2.0 * order[1:])))
    term = 0.5 * (np.log((2.0 * order + 1.0) / (4.0 * math.pi)) + steps)
    return np.repeat(term[:, None], 128, axis=1).astype(np.float32)


def degree_terms():
    degree = np.arange(LL, dtype=np.float64)
    return np.stack(
        [
            np.sqrt(np.maximum(4.0 * degree**2 - 1.0, 1.0)),
            1.0 / np.sqrt(np.maximum(4.0 * (degree - 1.0) ** 2 - 1.0, 1.0)),
        ]
    ).astype(np.float32)


def rows_kernel(x_ref, first_ref, last_ref):
    for u in range(2):
        first_ref[pl.ds(u * C, C), :] = x_ref[pl.ds(u, C, stride=TL), :].astype(BF16)
        last_ref[pl.ds(u * C, C), :] = x_ref[pl.ds(TL - 2 + u, C, stride=TL), :].astype(BF16)


def edges_kernel(core_ref, x_ref, up_ref, down_ref, far_ref, near_ref):
    row = lax.broadcasted_iota(jnp.int32, (64, JL), 0)
    lane = lax.broadcasted_iota(jnp.int32, (64, JL), 1)
    total = jnp.zeros((64, C), F32)
    for r in range(12):
        if r < 2:
            cells = up_ref[pl.ds(r * C, C), :]
        elif r < 10:
            cells = x_ref[pl.ds(r - 2, C, stride=TL), :].astype(BF16)
        else:
            cells = down_ref[pl.ds((r - 10) * C, C), :]
        head = (row - 2 * r == lane) & (lane < 2)
        tail = (row - 32 - 2 * r == lane - (JL - 2)) & (lane >= JL - 2)
        total = total + dot((head | tail).astype(F32).astype(BF16), cells, ((1,), (1,)))
    odd = core_ref[0] == 1
    far_ref[...] = jnp.where(odd, total[32:], total[:32]).astype(BF16)
    near_ref[...] = jnp.where(odd, total[:32], total[32:]).astype(BF16)


def weights_kernel(w_ref, mix_ref, norm_ref, wt_ref, mixt_ref, gain_ref):
    gain_ref[...] = jnp.broadcast_to(norm_ref[...], (JL, C)).T
    wt_ref[...] = w_ref[...].T
    mixt_ref[...] = mix_ref[...].T


def legendre_kernel(
    place_ref, degree_ref, term_ref, lat_ref, table_ref, left_ref, right_ref
):
    first = place_ref[0] * ORD
    order = (first + lax.broadcasted_iota(jnp.int32, (ORD, 128), 0)).astype(F32)
    squared = order * order
    term = term_ref[pl.ds(pl.multiple_of(first, ORD), ORD), :]
    cosines, seeds, undos = [], [], []
    for h in range(2):
        lanes = pl.ds(128 * h, 128)
        log_seed = term + order * lat_ref[pl.ds(1, 1), lanes]
        rescale = jnp.clip(-log_seed, 0.0, 80.0)
        cosines.append(jnp.broadcast_to(lat_ref[pl.ds(0, 1), lanes], (ORD, 128)))
        seeds.append(jnp.exp(log_seed + rescale))
        undos.append(jnp.exp(-rescale))
    refs = (left_ref, right_ref)

    def advance(degree, state):
        real = degree.astype(F32)
        below = real - 1.0
        a = degree_ref[0, degree] * lax.rsqrt(jnp.maximum(real * real - squared, 1.0))
        b = degree_ref[1, degree] * jnp.sqrt(jnp.maximum(below * below - squared, 0.0))
        found = []
        for h in range(2):
            last, before = state[2 * h], state[2 * h + 1]
            recurred = a * (cosines[h] * last - b * before)
            current = jnp.where(
                order == real, seeds[h], jnp.where(order < real, recurred, 0.0)
            )
            refs[h][pl.ds(pl.multiple_of(degree * ORD, ORD), ORD), :] = current * undos[h]
            found += [current, last]
        return tuple(found)

    empty = order * 0.0 * seeds[0]
    lax.fori_loop(0, LL, advance, (empty,) * 4, unroll=4)
    quad = lat_ref[pl.ds(2, 1), :]
    for m in range(ORD):
        table = jnp.concatenate(
            [left_ref[pl.ds(m, LL, stride=ORD), :], right_ref[pl.ds(m, LL, stride=ORD), :]], axis=1
        )
        table_ref[0, m] = (table * quad).astype(BF16)
        table_ref[1, m] = table.T.astype(BF16)


def conv_kernel(
    dlat_ref,
    dlon_ref,
    basis_ref,
    quad_ref,
    x_ref,
    up_ref,
    down_ref,
    wt_ref,
    after_ref,
    shifted_ref,
    sums_ref,
):
    lanes = lax.broadcasted_iota(jnp.int32, (C, JL), 1)
    for r in range(12):
        if r < 2:
            cells = up_ref[pl.ds(r * C, C), :].astype(F32)
        elif r < 10:
            cells = x_ref[pl.ds(r - 2, C, stride=TL), :]
        else:
            cells = down_ref[pl.ds((r - 10) * C, C), :].astype(F32)
        for s in range(5):
            by = s - 2
            if by > 0:
                moved = jnp.where(lanes < JL - by, pltpu.roll(cells, JL - by, 1), 0.0)
            elif by < 0:
                moved = jnp.where(lanes >= -by, pltpu.roll(cells, -by, 1), 0.0)
            else:
                moved = cells
            shifted_ref[s * 12 + r] = moved

    def one_row(t, carry):
        sums_ref[...] = jnp.zeros((NBASIS, C, JL), F32)
        for k in range(KSUP):
            b = basis_ref[t, k]
            place = (dlon_ref[t, k] + 2) * 12 + dlat_ref[t, k] + 2 + t
            sums_ref[b] = sums_ref[b] + quad_ref[t, k] * shifted_ref[place]
        aggregate = sums_ref[...].astype(BF16).reshape(NBASIS * C, JL)
        rows = pl.ds(t, C, stride=TL)
        after_ref[rows, :] = x_ref[rows, :] + dot(wt_ref[...], aggregate)
        return carry

    lax.fori_loop(0, TL, one_row, 0)


def seam_kernel(
    core_ref,
    dlat_ref,
    dlon_ref,
    basis_ref,
    quad_ref,
    inner_ref,
    far_ref,
    near_ref,
    wt_ref,
    gain_ref,
    after_ref,
    normed_ref,
    scaled_ref,
):
    even = core_ref[0] == 0
    far = far_ref[...].astype(F32)
    near = near_ref[...].astype(F32)
    west = jnp.where(even, far, near)
    east = jnp.where(even, near, far)
    edges = jnp.concatenate([west, east], axis=0).T.astype(BF16)
    row = lax.broadcasted_iota(jnp.int32, (64, 128), 0)
    lane = lax.broadcasted_iota(jnp.int32, (8, 128), 1)
    own = (lane >> 2) & 7
    col = lane & 3
    gather = jnp.zeros((64, 128), F32)
    for k in range(KSUP):
        dlat = jnp.zeros((8, 128), jnp.int32)
        dlon = dlat
        basis = dlat
        quad = jnp.zeros((8, 128), F32)
        for t in range(TL):
            here = own == t
            dlat = jnp.where(here, dlat_ref[t, k], dlat)
            dlon = jnp.where(here, dlon_ref[t, k], dlon)
            basis = jnp.where(here, basis_ref[t, k], basis)
            quad = jnp.where(here, quad_ref[t, k], quad)
        start = 2 * (own + 2 + dlat)
        cell = col + dlon
        source = jnp.where(
            col < 2,
            jnp.where(cell >= 2, 32 + start + cell - 2, -1),
            jnp.where(cell < 2, start + cell, -1),
        )
        source = jnp.where(basis == lane >> 5, source, -1)
        gather = gather + jnp.where(
            row == jnp.concatenate([source] * 8, axis=0), jnp.concatenate([quad] * 8, axis=0), 0.0
        )
    high, low = two_parts(gather)
    sums = dot(edges, high) + dot(edges, low)
    aggregate = jnp.concatenate(
        [sums.astype(BF16)]
        + [pltpu.roll(sums, 128 - 32 * b, 1).astype(BF16) for b in range(1, NBASIS)],
        axis=0,
    )
    seam = dot(wt_ref[...], aggregate)
    lanes = lax.broadcasted_iota(jnp.int32, (C, JL), 1)
    outer = (lanes < 2) | (lanes >= JL - 2)
    for t in range(TL):
        rows = pl.ds(t, C, stride=TL)
        moved = pltpu.roll(seam, (JL - 2 - 4 * t) % JL, 1)
        after = inner_ref[rows, :] + jnp.where(outer, moved, 0.0)
        after_ref[rows, :] = after
        inverse = lax.rsqrt(jnp.sum(after * after, axis=0, keepdims=True) * (1.0 / C) + 1e-6)
        scaled_ref[rows, :] = after * inverse * gain_ref[...]
    normed_ref[...] = scaled_ref[...].astype(BF16)


def fourier_kernel(recv_ref, hi_ref, lo_ref, lane_ref, out_ref):
    circles = jnp.concatenate(
        [
            jnp.concatenate([recv_ref[8 * y + s] for s in range(8)], axis=1)
            for y in range(4)
        ],
        axis=0,
    )
    dims = ((1,), (1,))
    found = dot(hi_ref[...], circles, dims) + dot(lo_ref[...], circles, dims)
    out_ref[...] = dot(found.astype(BF16), lane_ref[...]).astype(BF16)


def spectral_kernel(
    recv_ref, table_ref, filter_ref, out_ref, in_ref, rows_ref, back_ref
):
    first = pl.program_id(0) * STEP

    @pl.when(first == 0)
    def _():
        for j in range(3):
            in_ref[j] = recv_ref[:, 128 * j : 128 * (j + 1)].astype(F32)

    lane = lax.broadcasted_iota(jnp.int32, (8, 128), 1)
    for i in range(STEP):
        parts = []
        for r in range(2):
            for j in range(3):
                near = in_ref[j, pl.ds(r * ORD + first + i, 8, stride=32), :]
                far = in_ref[j, pl.ds(256 + r * ORD + first + i, 8, stride=32), :]
                parts.append(near - far if i % 2 else near + far)
        for yt in range(32):
            tile = None
            for n in range(6):
                moved = pltpu.roll(parts[n], (4 * n - 4 * yt) % 128, 1)
                tile = moved if tile is None else jnp.where(lane >= 4 * n, moved, tile)
            rows_ref[i, pl.ds(8 * yt, 8), :] = tile
    filtered = []
    for i in range(STEP):
        fields = rows_ref[i].astype(BF16)
        spectra = dot(table_ref[0, i], fields)
        filtered.append((spectra * filter_ref[...]).astype(BF16))
    for i in range(STEP):
        rows_ref[i] = dot(table_ref[1, i], filtered[i])
    for i in range(STEP):
        found = [None] * 6
        for yt in range(32):
            tile = rows_ref[i, pl.ds(8 * yt, 8), :]
            for n in range(6):
                moved = pltpu.roll(tile, (4 * yt - 4 * n) % 128, 1)
                found[n] = moved if yt == 0 else jnp.where(lane >= 4 * yt, moved, found[n])
        for r in range(2):
            for j in range(3):
                value = found[3 * r + j]
                back_ref[j, pl.ds(r * ORD + first + i, 8, stride=32), :] = value
                back_ref[j, pl.ds(256 + r * ORD + first + i, 8, stride=32), :] = (
                    -value if i % 2 else value
                )

    @pl.when(first == ORD - STEP)
    def _():
        for j in range(3):
            out_ref[:, 128 * j : 128 * (j + 1)] = back_ref[j].astype(BF16)


def inverse_kernel(recv_ref, hi_ref, lo_ref, lane_ref, out_ref):
    turned = dot(lane_ref[...], recv_ref[...], ((1,), (1,))).astype(BF16)
    for s in range(8):
        lons = pl.ds(128 * s, 128)
        wave = dot(turned, hi_ref[:, lons]) + dot(turned, lo_ref[:, lons])
        act = jax.nn.gelu(wave, approximate=True).astype(BF16)
        for y in range(4):
            out_ref[8 * y + s] = act[96 * y : 96 * (y + 1)]


def mix_kernel(act_ref, after_ref, mixt_ref, out_ref, wide_ref):
    wide_ref[...] = act_ref[...].astype(F32)
    for t in range(TL):
        rows = pl.ds(t, C, stride=TL)
        mixed = dot(mixt_ref[...], wide_ref[rows, :].astype(BF16))
        out_ref[rows, :] = after_ref[rows, :] + mixed


def exchanged(blocks, axes):
    return lax.all_to_all(blocks, axes, split_axis=0, concat_axis=0, tiled=True)


def pairs(count, first):
    ends = [(i, (i + 1) % count) for i in range(first, count, 2)]
    return ends + [(j, i) for i, j in ends]


def per_device(
    grid_field,
    disco_dlat,
    disco_dlon,
    disco_basis,
    disco_quad,
    disco_weight,
    norm_gain,
    spectral_filter,
    mix_weight,
):
    (fwd_hi, fwd_lo), (inv_hi, inv_lo) = longitude_tables()
    lanes = lane_order()
    smem = pl.BlockSpec(memory_space=pltpu.SMEM)
    vmem = pl.BlockSpec(memory_space=pltpu.VMEM)
    x = grid_field.reshape(C * TL, JL)

    lat_count = lax.axis_size(LAT)
    lon_count = lax.axis_size(LON)
    first, last = call(rows_kernel, "rows", 6, (shape((2 * C, JL)), shape((2 * C, JL))))(x)
    up = lax.ppermute(last, LAT, [(i, i + 1) for i in range(lat_count - 1)])
    down = lax.ppermute(first, LAT, [(i + 1, i) for i in range(lat_count - 1)])
    wt, mixt, gain = call(
        weights_kernel,
        "weights",
        10,
        (shape((C, NBASIS * C)), shape((C, C)), shape((C, JL), F32)),
    )(disco_weight.reshape(NBASIS * C, C), mix_weight, norm_gain.reshape(1, C))
    own = lax.dynamic_slice_in_dim(spectral_filter, lax.axis_index(CHAN) * CB, CB, 0)
    own = jnp.concatenate([own, own, jnp.zeros((128 - 2 * CB, LL), F32)], axis=0).T
    up, down, wt, mixt, gain, own = lax.optimization_barrier((up, down, wt, mixt, gain, own))
    core = lax.axis_index("core").astype(jnp.int32).reshape(1)
    far, near = call(
        edges_kernel, "edges", 6, (shape((32, C)), shape((32, C))), in_specs=[smem] + [vmem] * 3
    )(core, x, up, down)
    far = lax.ppermute(far, LON, pairs(lon_count, 1))
    near = lax.ppermute(near, LON, pairs(lon_count, 0))

    place = lax.axis_index(RING).astype(jnp.int32).reshape(1)
    tables = call(
        legendre_kernel,
        "legendre", 57,
        shape((2, ORD, LL, NLAT)),
        in_specs=[smem, smem, vmem, vmem],
        scratch=(pltpu.VMEM((LL * ORD, 128), F32), pltpu.VMEM((LL * ORD, 128), F32)),
    )(place, degree_terms(), order_terms(), latitude_rows())
    tables = pltpu.with_memory_space_constraint(tables, pltpu.HBM)

    inner = call(
        conv_kernel,
        "conv", 24,
        shape((C * TL, JL), F32),
        in_specs=[smem] * 4 + [vmem] * 4,
        scratch=(pltpu.VMEM((60, C, JL), F32), pltpu.VMEM((NBASIS, C, JL), F32)),
    )(disco_dlat, disco_dlon, disco_basis, disco_quad, x, up, down, wt)
    after, normed = call(
        seam_kernel,
        "seam", 12,
        (shape((C * TL, JL), F32), shape((C * TL, JL))),
        in_specs=[smem] * 5 + [vmem] * 5,
        scratch=(pltpu.VMEM((C * TL, JL), F32),),
    )(core, disco_dlat, disco_dlon, disco_basis, disco_quad, inner, far, near, wt, gain)

    portion = exchanged(normed.reshape(32, CB * TL, JL), CHAN)
    fourier = call(fourier_kernel, "fourier", 16, shape((2 * MM, C)))(portion, fwd_hi, fwd_lo, lanes)
    gathered = exchanged(fourier.reshape(16, 2 * ORD, C), RING)
    whole = pl.BlockSpec((2 * MM, C), lambda m: (0, 0))
    table = pl.BlockSpec((2, STEP, LL, NLAT), lambda m: (0, m, 0, 0))
    synthesis = call(
        spectral_kernel,
        "spectral", 14,
        shape((2 * MM, C)),
        grid=(ORD // STEP,),
        in_specs=[whole, table, pl.BlockSpec((LL, 128), lambda m: (0, 0))],
        out_specs=whole,
        scratch=(
            pltpu.VMEM((3, 2 * MM, 128), F32),
            pltpu.VMEM((STEP, NLAT, 128), F32),
            pltpu.VMEM((3, 2 * MM, 128), F32),
        ),
    )(gathered.reshape(2 * MM, C), tables, own)
    returned = exchanged(synthesis.reshape(16, 2 * ORD, C), RING)
    activated = call(inverse_kernel, "inverse", 16, shape((32, CB * TL, JL)))(
        returned.reshape(2 * MM, C), inv_hi, inv_lo, lanes
    )
    mixed = exchanged(activated, CHAN)
    out = call(
        mix_kernel, "mix", 12, shape((C * TL, JL), F32), scratch=(pltpu.VMEM((C * TL, JL), F32),)
    )(mixed.reshape(C * TL, JL), after, mixt)
    return out.reshape(C, TL, JL)


def solution(mesh):
    torus = Mesh(mesh.devices.reshape(8, 4, 2, 4, 2), ("zl", "y", "zh", "x", "core"))
    placed = (P(None, LAT, LON),) + (P(LAT, None),) * 4 + (P(),) * 4
    return jax.shard_map(
        per_device, mesh=torus, in_specs=placed, out_specs=P(None, LAT, LON), check_vma=False
    )
```

```python
import math

import jax
import jax.numpy as jnp
import numpy as np
from jax import lax
from jax.experimental import pallas as pl
from jax.experimental.pallas import tpu as pltpu
from jax.sharding import Mesh
from jax.sharding import PartitionSpec as P

C = 384
NLAT = 256
NLON = 2048
MM = 256
LL = 256
KSUP = 16
NBASIS = 4
TL = 8
JL = 128
CB = 12
ORD = 16
STEP = 4
LAT = ("zl", "y")
LON = ("zh", "x", "core")
CHAN = ("y", "x", "core")
RING = ("zh", "zl")
F32 = jnp.float32
BF16 = jnp.bfloat16


def call(kernel, name, mib, out_shape, in_specs=None, scratch=(), grid=None, out_specs=None):
    kwargs = {}
    if grid is not None:
        kwargs["grid"] = grid
    if in_specs is not None:
        kwargs["in_specs"] = in_specs
    if out_specs is not None:
        kwargs["out_specs"] = out_specs
    return pl.pallas_call(
        kernel,
        out_shape=out_shape,
        scratch_shapes=list(scratch),
        name=name,
        compiler_params=pltpu.CompilerParams(vmem_limit_bytes=mib * 1024 * 1024),
        **kwargs,
    )


def shape(dims, kind=BF16):
    return jax.ShapeDtypeStruct(dims, kind)


def dot(a, b, dims=((1,), (0,))):
    return lax.dot_general(a, b, (dims, ((), ())), preferred_element_type=F32)


def two_parts(value):
    high = value.astype(BF16)
    return high, (value - high.astype(F32)).astype(BF16)


def longitude_tables():
    order = np.arange(MM)
    lon = np.arange(NLON // 2)
    phase = (order[:, None] * lon[None, :] % NLON) * (2.0 * math.pi / NLON)
    cosine, sine = np.cos(phase), -np.sin(phase)
    both = np.stack([cosine, sine]).reshape(2, MM // ORD, ORD, NLON // 2)
    both = both.transpose(1, 0, 2, 3).reshape(2 * MM, NLON // 2)
    weight = np.where(order == 0, 1.0, 2.0).reshape(MM // ORD, 1, ORD)
    weight = np.broadcast_to(weight, (MM // ORD, 2, ORD)).reshape(2 * MM, 1)
    forward = both * (2.0 * math.pi / NLON)
    return forward.astype(jnp.bfloat16), (both * weight).astype(jnp.bfloat16)


def lane_order():
    y, c, t = np.meshgrid(np.arange(4), np.arange(CB), np.arange(TL), indexing="ij")
    src = (y * CB + c) * TL + t
    dst = ((c // 4 * 4 + y) * TL + t) * 4 + c % 4
    out = np.zeros((4 * CB * TL, 4 * CB * TL), np.float32)
    out[src.ravel(), dst.ravel()] = 1.0
    return out.astype(jnp.bfloat16)


def latitude_rows():
    lane = np.arange(NLAT)
    lat = lane % 8 * 32 + lane // 8
    colat = math.pi * (lat + 0.5) / NLAT
    rows = np.zeros((8, NLAT), np.float32)
    rows[0] = np.cos(colat)
    rows[1] = np.log(np.sin(colat))
    rows[2] = math.pi / NLAT * np.sin(colat)
    return rows


def order_terms():
    order = np.arange(MM, dtype=np.float64)
    steps = np.zeros(MM)
    steps[1:] = np.cumsum(np.log((2.0 * order[1:] - 1.0) / (2.0 * order[1:])))
    term = 0.5 * (np.log((2.0 * order + 1.0) / (4.0 * math.pi)) + steps)
    return np.repeat(term[:, None], 128, axis=1).astype(np.float32)


def degree_terms():
    degree = np.arange(LL, dtype=np.float64)
    return np.stack(
        [
            np.sqrt(np.maximum(4.0 * degree**2 - 1.0, 1.0)),
            1.0 / np.sqrt(np.maximum(4.0 * (degree - 1.0) ** 2 - 1.0, 1.0)),
        ]
    ).astype(np.float32)


def rows_kernel(x_ref, first_ref, last_ref):
    for u in range(2):
        first_ref[pl.ds(u * C, C), :] = x_ref[pl.ds(u, C, stride=TL), :].astype(BF16)
        last_ref[pl.ds(u * C, C), :] = x_ref[pl.ds(TL - 2 + u, C, stride=TL), :].astype(BF16)


def edges_kernel(core_ref, x_ref, up_ref, down_ref, far_ref, near_ref):
    row = lax.broadcasted_iota(jnp.int32, (64, JL), 0)
    lane = lax.broadcasted_iota(jnp.int32, (64, JL), 1)
    total = jnp.zeros((64, C), F32)
    for r in range(12):
        if r < 2:
            cells = up_ref[pl.ds(r * C, C), :]
        elif r < 10:
            cells = x_ref[pl.ds(r - 2, C, stride=TL), :].astype(BF16)
        else:
            cells = down_ref[pl.ds((r - 10) * C, C), :]
        head = (row - 2 * r == lane) & (lane < 2)
        tail = (row - 32 - 2 * r == lane - (JL - 2)) & (lane >= JL - 2)
        total = total + dot((head | tail).astype(F32).astype(BF16), cells, ((1,), (1,)))
    odd = core_ref[0] == 1
    far_ref[...] = jnp.where(odd, total[32:], total[:32]).astype(BF16)
    near_ref[...] = jnp.where(odd, total[:32], total[32:]).astype(BF16)


def weights_kernel(w_ref, mix_ref, norm_ref, wt_ref, mixt_ref, gain_ref):
    gain_ref[...] = jnp.broadcast_to(norm_ref[...], (JL, C)).T
    wt_ref[...] = w_ref[...].T
    mixt_ref[...] = mix_ref[...].T


def legendre_kernel(
    place_ref, degree_ref, term_ref, lat_ref, table_ref, left_ref, right_ref
):
    first = place_ref[0] * ORD
    order = (first + lax.broadcasted_iota(jnp.int32, (ORD, 128), 0)).astype(F32)
    squared = order * order
    term = term_ref[pl.ds(pl.multiple_of(first, ORD), ORD), :]
    cosines, seeds, undos = [], [], []
    for h in range(2):
        lanes = pl.ds(128 * h, 128)
        log_seed = term + order * lat_ref[pl.ds(1, 1), lanes]
        rescale = jnp.clip(-log_seed, 0.0, 80.0)
        cosines.append(jnp.broadcast_to(lat_ref[pl.ds(0, 1), lanes], (ORD, 128)))
        seeds.append(jnp.exp(log_seed + rescale))
        undos.append(jnp.exp(-rescale))
    refs = (left_ref, right_ref)

    def advance(degree, state):
        real = degree.astype(F32)
        below = real - 1.0
        a = degree_ref[0, degree] * lax.rsqrt(jnp.maximum(real * real - squared, 1.0))
        b = degree_ref[1, degree] * jnp.sqrt(jnp.maximum(below * below - squared, 0.0))
        found = []
        for h in range(2):
            last, before = state[2 * h], state[2 * h + 1]
            recurred = a * (cosines[h] * last - b * before)
            current = jnp.where(
                order == real, seeds[h], jnp.where(order < real, recurred, 0.0)
            )
            refs[h][pl.ds(pl.multiple_of(degree * ORD, ORD), ORD), :] = current * undos[h]
            found += [current, last]
        return tuple(found)

    empty = order * 0.0 * seeds[0]
    lax.fori_loop(0, LL, advance, (empty,) * 4, unroll=4)
    quad = lat_ref[pl.ds(2, 1), :]
    for m in range(ORD):
        table = jnp.concatenate(
            [left_ref[pl.ds(m, LL, stride=ORD), :], right_ref[pl.ds(m, LL, stride=ORD), :]], axis=1
        )
        table_ref[0, m] = (table * quad).astype(BF16)
        table_ref[1, m] = table.T.astype(BF16)


def conv_kernel(
    dlat_ref,
    dlon_ref,
    basis_ref,
    quad_ref,
    x_ref,
    up_ref,
    down_ref,
    wt_ref,
    after_ref,
    shifted_ref,
    sums_ref,
):
    lanes = lax.broadcasted_iota(jnp.int32, (C, JL), 1)
    for r in range(12):
        if r < 2:
            cells = up_ref[pl.ds(r * C, C), :].astype(F32)
        elif r < 10:
            cells = x_ref[pl.ds(r - 2, C, stride=TL), :]
        else:
            cells = down_ref[pl.ds((r - 10) * C, C), :].astype(F32)
        for s in range(5):
            by = s - 2
            if by > 0:
                moved = jnp.where(lanes < JL - by, pltpu.roll(cells, JL - by, 1), 0.0)
            elif by < 0:
                moved = jnp.where(lanes >= -by, pltpu.roll(cells, -by, 1), 0.0)
            else:
                moved = cells
            shifted_ref[s * 12 + r] = moved

    def one_row(t, carry):
        sums_ref[...] = jnp.zeros((NBASIS, C, JL), F32)
        for k in range(KSUP):
            b = basis_ref[t, k]
            place = (dlon_ref[t, k] + 2) * 12 + dlat_ref[t, k] + 2 + t
            sums_ref[b] = sums_ref[b] + quad_ref[t, k] * shifted_ref[place]
        aggregate = sums_ref[...].astype(BF16).reshape(NBASIS * C, JL)
        rows = pl.ds(t, C, stride=TL)
        after_ref[rows, :] = x_ref[rows, :] + dot(wt_ref[...], aggregate)
        return carry

    lax.fori_loop(0, TL, one_row, 0)


def seam_kernel(
    core_ref,
    dlat_ref,
    dlon_ref,
    basis_ref,
    quad_ref,
    inner_ref,
    far_ref,
    near_ref,
    wt_ref,
    gain_ref,
    after_ref,
    normed_ref,
    scaled_ref,
):
    even = core_ref[0] == 0
    far = far_ref[...].astype(F32)
    near = near_ref[...].astype(F32)
    west = jnp.where(even, far, near)
    east = jnp.where(even, near, far)
    edges = jnp.concatenate([west, east], axis=0).T.astype(BF16)
    row = lax.broadcasted_iota(jnp.int32, (64, 128), 0)
    lane = lax.broadcasted_iota(jnp.int32, (8, 128), 1)
    own = (lane >> 2) & 7
    col = lane & 3
    gather = jnp.zeros((64, 128), F32)
    for k in range(KSUP):
        dlat = jnp.zeros((8, 128), jnp.int32)
        dlon = dlat
        basis = dlat
        quad = jnp.zeros((8, 128), F32)
        for t in range(TL):
            here = own == t
            dlat = jnp.where(here, dlat_ref[t, k], dlat)
            dlon = jnp.where(here, dlon_ref[t, k], dlon)
            basis = jnp.where(here, basis_ref[t, k], basis)
            quad = jnp.where(here, quad_ref[t, k], quad)
        start = 2 * (own + 2 + dlat)
        cell = col + dlon
        source = jnp.where(
            col < 2,
            jnp.where(cell >= 2, 32 + start + cell - 2, -1),
            jnp.where(cell < 2, start + cell, -1),
        )
        source = jnp.where(basis == lane >> 5, source, -1)
        gather = gather + jnp.where(
            row == jnp.concatenate([source] * 8, axis=0), jnp.concatenate([quad] * 8, axis=0), 0.0
        )
    high, low = two_parts(gather)
    sums = dot(edges, high) + dot(edges, low)
    aggregate = jnp.concatenate(
        [sums.astype(BF16)]
        + [pltpu.roll(sums, 128 - 32 * b, 1).astype(BF16) for b in range(1, NBASIS)],
        axis=0,
    )
    seam = dot(wt_ref[...], aggregate)
    lanes = lax.broadcasted_iota(jnp.int32, (C, JL), 1)
    outer = (lanes < 2) | (lanes >= JL - 2)
    for t in range(TL):
        rows = pl.ds(t, C, stride=TL)
        moved = pltpu.roll(seam, (JL - 2 - 4 * t) % JL, 1)
        after = inner_ref[rows, :] + jnp.where(outer, moved, 0.0)
        after_ref[rows, :] = after
        inverse = lax.rsqrt(jnp.sum(after * after, axis=0, keepdims=True) * (1.0 / C) + 1e-6)
        scaled_ref[rows, :] = after * inverse * gain_ref[...]
    normed_ref[...] = scaled_ref[...].astype(BF16)


def fourier_kernel(recv_ref, lon_ref, lane_ref, out_ref):
    circles = jnp.concatenate(
        [
            jnp.concatenate([recv_ref[8 * y + s] for s in range(8)], axis=1)
            for y in range(4)
        ],
        axis=0,
    )
    found = dot(lon_ref[...], circles, ((1,), (1,)))
    out_ref[...] = dot(found.astype(BF16), lane_ref[...]).astype(BF16)


def spectral_kernel(
    recv_ref, table_ref, filter_ref, out_ref, in_ref, rows_ref, back_ref
):
    first = pl.program_id(0) * STEP

    @pl.when(first == 0)
    def _():
        for j in range(3):
            in_ref[j] = recv_ref[:, 128 * j : 128 * (j + 1)].astype(F32)

    block = lax.broadcasted_iota(jnp.int32, (8, 128), 1) >> 2
    orders = []
    for i in range(STEP):
        parts = []
        for r in range(2):
            for j in range(3):
                near = in_ref[j, pl.ds(r * ORD + first + i, 8, stride=32), :]
                far = in_ref[j, pl.ds(256 + r * ORD + first + i, 8, stride=32), :]
                part = near - far if i % 2 else near + far
                parts.append(pltpu.roll(part, 12 * r + 4 * j, 1) if r + j else part)
        orders.append(parts)
    for yt in range(32):
        place = (block - yt) & 31
        for i in range(STEP):
            tile = orders[i][0]
            for n in range(1, 6):
                tile = jnp.where(place >= n, orders[i][n], tile)
            rows_ref[i, pl.ds(8 * yt, 8), :] = pltpu.roll(tile, 128 - 4 * yt, 1) if yt else tile
    filtered = []
    for i in range(STEP):
        fields = rows_ref[i].astype(BF16)
        spectra = dot(table_ref[0, i], fields)
        filtered.append((spectra * filter_ref[...]).astype(BF16))
    for i in range(STEP):
        rows_ref[i] = dot(table_ref[1, i], filtered[i])
    found = [[None] * 6 for i in range(STEP)]
    for yt in range(32):
        place = (block - yt) & 31
        for i in range(STEP):
            tile = rows_ref[i, pl.ds(8 * yt, 8), :]
            if yt:
                tile = pltpu.roll(tile, 4 * yt, 1)
            for n in range(6):
                found[i][n] = jnp.where(place == n, tile, found[i][n]) if yt else tile
    for i in range(STEP):
        for r in range(2):
            for j in range(3):
                value = found[i][3 * r + j]
                if r + j:
                    value = pltpu.roll(value, 128 - 12 * r - 4 * j, 1)
                back_ref[j, pl.ds(r * ORD + first + i, 8, stride=32), :] = value
                back_ref[j, pl.ds(256 + r * ORD + first + i, 8, stride=32), :] = (
                    -value if i % 2 else value
                )

    @pl.when(first == ORD - STEP)
    def _():
        for j in range(3):
            out_ref[:, 128 * j : 128 * (j + 1)] = back_ref[j].astype(BF16)


def inverse_kernel(recv_ref, lon_ref, lane_ref, out_ref):
    turned = dot(lane_ref[...], recv_ref[...], ((1,), (1,))).astype(BF16)
    for s in range(8):
        lons = pl.ds(128 * s, 128)
        wave = dot(turned, lon_ref[:, lons])
        act = jax.nn.gelu(wave, approximate=True).astype(BF16)
        for y in range(4):
            out_ref[8 * y + s] = act[96 * y : 96 * (y + 1)]


def mix_kernel(act_ref, after_ref, mixt_ref, out_ref, wide_ref):
    wide_ref[...] = act_ref[...].astype(F32)
    for t in range(TL):
        rows = pl.ds(t, C, stride=TL)
        mixed = dot(mixt_ref[...], wide_ref[rows, :].astype(BF16))
        out_ref[rows, :] = after_ref[rows, :] + mixed


def exchanged(blocks, axes):
    return lax.all_to_all(blocks, axes, split_axis=0, concat_axis=0, tiled=True)


def pairs(count, first):
    ends = [(i, (i + 1) % count) for i in range(first, count, 2)]
    return ends + [(j, i) for i, j in ends]


def per_device(
    grid_field,
    disco_dlat,
    disco_dlon,
    disco_basis,
    disco_quad,
    disco_weight,
    norm_gain,
    spectral_filter,
    mix_weight,
):
    forward, backward = longitude_tables()
    lanes = lane_order()
    smem = pl.BlockSpec(memory_space=pltpu.SMEM)
    vmem = pl.BlockSpec(memory_space=pltpu.VMEM)
    x = grid_field.reshape(C * TL, JL)

    lat_count = lax.axis_size(LAT)
    lon_count = lax.axis_size(LON)
    first, last = call(rows_kernel, "rows", 6, (shape((2 * C, JL)), shape((2 * C, JL))))(x)
    up = lax.ppermute(last, LAT, [(i, i + 1) for i in range(lat_count - 1)])
    down = lax.ppermute(first, LAT, [(i + 1, i) for i in range(lat_count - 1)])
    wt, mixt, gain = call(
        weights_kernel,
        "weights",
        10,
        (shape((C, NBASIS * C)), shape((C, C)), shape((C, JL), F32)),
    )(disco_weight.reshape(NBASIS * C, C), mix_weight, norm_gain.reshape(1, C))
    own = lax.dynamic_slice_in_dim(spectral_filter, lax.axis_index(CHAN) * CB, CB, 0)
    own = jnp.concatenate([own, own, jnp.zeros((128 - 2 * CB, LL), F32)], axis=0).T
    up, down, wt, mixt, gain, own = lax.optimization_barrier((up, down, wt, mixt, gain, own))
    core = lax.axis_index("core").astype(jnp.int32).reshape(1)
    far, near = call(
        edges_kernel, "edges", 6, (shape((32, C)), shape((32, C))), in_specs=[smem] + [vmem] * 3
    )(core, x, up, down)
    far = lax.ppermute(far, LON, pairs(lon_count, 1))
    near = lax.ppermute(near, LON, pairs(lon_count, 0))

    place = lax.axis_index(RING).astype(jnp.int32).reshape(1)
    tables = call(
        legendre_kernel,
        "legendre", 57,
        shape((2, ORD, LL, NLAT)),
        in_specs=[smem, smem, vmem, vmem],
        scratch=(pltpu.VMEM((LL * ORD, 128), F32), pltpu.VMEM((LL * ORD, 128), F32)),
    )(place, degree_terms(), order_terms(), latitude_rows())
    tables = pltpu.with_memory_space_constraint(tables, pltpu.HBM)

    inner = call(
        conv_kernel,
        "conv", 24,
        shape((C * TL, JL), F32),
        in_specs=[smem] * 4 + [vmem] * 4,
        scratch=(pltpu.VMEM((60, C, JL), F32), pltpu.VMEM((NBASIS, C, JL), F32)),
    )(disco_dlat, disco_dlon, disco_basis, disco_quad, x, up, down, wt)
    after, normed = call(
        seam_kernel,
        "seam", 12,
        (shape((C * TL, JL), F32), shape((C * TL, JL))),
        in_specs=[smem] * 5 + [vmem] * 5,
        scratch=(pltpu.VMEM((C * TL, JL), F32),),
    )(core, disco_dlat, disco_dlon, disco_basis, disco_quad, inner, far, near, wt, gain)

    portion = exchanged(normed.reshape(32, CB * TL, JL), CHAN)
    fourier = call(fourier_kernel, "fourier", 16, shape((2 * MM, C)))(portion, forward, lanes)
    gathered = exchanged(fourier.reshape(16, 2 * ORD, C), RING)
    whole = pl.BlockSpec((2 * MM, C), lambda m: (0, 0))
    table = pl.BlockSpec((2, STEP, LL, NLAT), lambda m: (0, m, 0, 0))
    synthesis = call(
        spectral_kernel,
        "spectral", 14,
        shape((2 * MM, C)),
        grid=(ORD // STEP,),
        in_specs=[whole, table, pl.BlockSpec((LL, 128), lambda m: (0, 0))],
        out_specs=whole,
        scratch=(
            pltpu.VMEM((3, 2 * MM, 128), F32),
            pltpu.VMEM((STEP, NLAT, 128), F32),
            pltpu.VMEM((3, 2 * MM, 128), F32),
        ),
    )(gathered.reshape(2 * MM, C), tables, own)
    returned = exchanged(synthesis.reshape(16, 2 * ORD, C), RING)
    activated = call(inverse_kernel, "inverse", 16, shape((32, CB * TL, JL)))(
        returned.reshape(2 * MM, C), backward, lanes
    )
    mixed = exchanged(activated, CHAN)
    out = call(
        mix_kernel, "mix", 12, shape((C * TL, JL), F32), scratch=(pltpu.VMEM((C * TL, JL), F32),)
    )(mixed.reshape(C * TL, JL), after, mixt)
    return out.reshape(C, TL, JL)


def solution(mesh):
    torus = Mesh(mesh.devices.reshape(8, 4, 2, 4, 2), ("zl", "y", "zh", "x", "core"))
    placed = (P(None, LAT, LON),) + (P(LAT, None),) * 4 + (P(),) * 4
    return jax.shard_map(
        per_device, mesh=torus, in_specs=placed, out_specs=P(None, LAT, LON), check_vma=False
    )
```

```python
import math

import jax
import jax.numpy as jnp
import numpy as np
from jax import lax
from jax.experimental import pallas as pl
from jax.experimental.pallas import tpu as pltpu
from jax.sharding import Mesh
from jax.sharding import PartitionSpec as P

C = 384
NLAT = 256
NLON = 2048
MM = 256
LL = 256
KSUP = 16
NBASIS = 4
TL = 8
JL = 128
CB = 12
ORD = 16
STEP = 4
LAT = ("zl", "y")
LON = ("zh", "x", "core")
CHAN = ("x", "y", "core")
RING = ("zh", "zl")
F32 = jnp.float32
BF16 = jnp.bfloat16


def call(kernel, name, mib, out_shape, in_specs=None, scratch=(), grid=None, out_specs=None):
    kwargs = {}
    if grid is not None:
        kwargs["grid"] = grid
    if in_specs is not None:
        kwargs["in_specs"] = in_specs
    if out_specs is not None:
        kwargs["out_specs"] = out_specs
    return pl.pallas_call(
        kernel,
        out_shape=out_shape,
        scratch_shapes=list(scratch),
        name=name,
        compiler_params=pltpu.CompilerParams(vmem_limit_bytes=mib * 1024 * 1024),
        **kwargs,
    )


def shape(dims, kind=BF16):
    return jax.ShapeDtypeStruct(dims, kind)


def dot(a, b, dims=((1,), (0,))):
    return lax.dot_general(a, b, (dims, ((), ())), preferred_element_type=F32)


def two_parts(value):
    high = value.astype(BF16)
    return high, (value - high.astype(F32)).astype(BF16)


def longitude_tables():
    order = np.arange(MM)
    lon = np.arange(NLON // 2)
    phase = (order[:, None] * lon[None, :] % NLON) * (2.0 * math.pi / NLON)
    cosine, sine = np.cos(phase), -np.sin(phase)
    both = np.stack([cosine, sine]).reshape(2, MM // ORD, ORD, NLON // 2)
    both = both.transpose(1, 0, 2, 3).reshape(2 * MM, NLON // 2)
    weight = np.where(order == 0, 1.0, 2.0).reshape(MM // ORD, 1, ORD)
    weight = np.broadcast_to(weight, (MM // ORD, 2, ORD)).reshape(2 * MM, 1)
    forward = both * (2.0 * math.pi / NLON)
    return forward.astype(jnp.bfloat16), (both * weight).astype(jnp.bfloat16)


def lane_order():
    y, c, t = np.meshgrid(np.arange(4), np.arange(CB), np.arange(TL), indexing="ij")
    src = (y * CB + c) * TL + t
    dst = ((c // 4 * 4 + y) * TL + t) * 4 + c % 4
    out = np.zeros((4 * CB * TL, 4 * CB * TL), np.float32)
    out[src.ravel(), dst.ravel()] = 1.0
    return out.astype(jnp.bfloat16)


def latitude_rows():
    lane = np.arange(NLAT)
    lat = lane % 8 * 32 + lane // 8
    colat = math.pi * (lat + 0.5) / NLAT
    rows = np.zeros((8, NLAT), np.float32)
    rows[0] = np.cos(colat)
    rows[1] = np.log(np.sin(colat))
    rows[2] = math.pi / NLAT * np.sin(colat)
    return rows


def order_terms():
    order = np.arange(MM, dtype=np.float64)
    steps = np.zeros(MM)
    steps[1:] = np.cumsum(np.log((2.0 * order[1:] - 1.0) / (2.0 * order[1:])))
    term = 0.5 * (np.log((2.0 * order + 1.0) / (4.0 * math.pi)) + steps)
    return np.repeat(term[:, None], 128, axis=1).astype(np.float32)


def degree_terms():
    degree = np.arange(LL, dtype=np.float64)
    return np.stack(
        [
            np.sqrt(np.maximum(4.0 * degree**2 - 1.0, 1.0)),
            1.0 / np.sqrt(np.maximum(4.0 * (degree - 1.0) ** 2 - 1.0, 1.0)),
        ]
    ).astype(np.float32)


def rows_kernel(x_ref, first_ref, last_ref):
    for u in range(2):
        first_ref[pl.ds(u * C, C), :] = x_ref[pl.ds(u, C, stride=TL), :].astype(BF16)
        last_ref[pl.ds(u * C, C), :] = x_ref[pl.ds(TL - 2 + u, C, stride=TL), :].astype(BF16)


def edges_kernel(core_ref, x_ref, up_ref, down_ref, far_ref, near_ref):
    row = lax.broadcasted_iota(jnp.int32, (64, JL), 0)
    lane = lax.broadcasted_iota(jnp.int32, (64, JL), 1)
    total = jnp.zeros((64, C), F32)
    for r in range(12):
        if r < 2:
            cells = up_ref[pl.ds(r * C, C), :]
        elif r < 10:
            cells = x_ref[pl.ds(r - 2, C, stride=TL), :].astype(BF16)
        else:
            cells = down_ref[pl.ds((r - 10) * C, C), :]
        head = (row - 2 * r == lane) & (lane < 2)
        tail = (row - 32 - 2 * r == lane - (JL - 2)) & (lane >= JL - 2)
        total = total + dot((head | tail).astype(F32).astype(BF16), cells, ((1,), (1,)))
    odd = core_ref[0] == 1
    far_ref[...] = jnp.where(odd, total[32:], total[:32]).astype(BF16)
    near_ref[...] = jnp.where(odd, total[:32], total[32:]).astype(BF16)


def weights_kernel(w_ref, mix_ref, norm_ref, wt_ref, mixt_ref, gain_ref):
    gain_ref[...] = jnp.broadcast_to(norm_ref[...], (JL, C)).T
    wt_ref[...] = w_ref[...].T
    mixt_ref[...] = mix_ref[...].T


def legendre_kernel(
    place_ref, degree_ref, term_ref, lat_ref, table_ref, left_ref, right_ref
):
    first = place_ref[0] * ORD
    order = (first + lax.broadcasted_iota(jnp.int32, (ORD, 128), 0)).astype(F32)
    squared = order * order
    term = term_ref[pl.ds(pl.multiple_of(first, ORD), ORD), :]
    cosines, seeds, undos = [], [], []
    for h in range(2):
        lanes = pl.ds(128 * h, 128)
        log_seed = term + order * lat_ref[pl.ds(1, 1), lanes]
        rescale = jnp.clip(-log_seed, 0.0, 80.0)
        cosines.append(jnp.broadcast_to(lat_ref[pl.ds(0, 1), lanes], (ORD, 128)))
        seeds.append(jnp.exp(log_seed + rescale))
        undos.append(jnp.exp(-rescale))
    refs = (left_ref, right_ref)

    def advance(degree, state):
        real = degree.astype(F32)
        below = real - 1.0
        a = degree_ref[0, degree] * lax.rsqrt(jnp.maximum(real * real - squared, 1.0))
        b = degree_ref[1, degree] * jnp.sqrt(jnp.maximum(below * below - squared, 0.0))
        found = []
        for h in range(2):
            last, before = state[2 * h], state[2 * h + 1]
            recurred = a * (cosines[h] * last - b * before)
            current = jnp.where(
                order == real, seeds[h], jnp.where(order < real, recurred, 0.0)
            )
            refs[h][pl.ds(pl.multiple_of(degree * ORD, ORD), ORD), :] = current * undos[h]
            found += [current, last]
        return tuple(found)

    empty = order * 0.0 * seeds[0]
    lax.fori_loop(0, LL, advance, (empty,) * 4, unroll=4)
    quad = lat_ref[pl.ds(2, 1), :]
    for m in range(ORD):
        table = jnp.concatenate(
            [left_ref[pl.ds(m, LL, stride=ORD), :], right_ref[pl.ds(m, LL, stride=ORD), :]], axis=1
        )
        table_ref[0, m] = (table * quad).astype(BF16)
        table_ref[1, m] = table.T.astype(BF16)


def conv_kernel(
    dlat_ref,
    dlon_ref,
    basis_ref,
    quad_ref,
    x_ref,
    up_ref,
    down_ref,
    wt_ref,
    after_ref,
    shifted_ref,
    sums_ref,
):
    lanes = lax.broadcasted_iota(jnp.int32, (C, JL), 1)
    for r in range(12):
        if r < 2:
            cells = up_ref[pl.ds(r * C, C), :].astype(F32)
        elif r < 10:
            cells = x_ref[pl.ds(r - 2, C, stride=TL), :]
        else:
            cells = down_ref[pl.ds((r - 10) * C, C), :].astype(F32)
        for s in range(5):
            by = s - 2
            if by > 0:
                moved = jnp.where(lanes < JL - by, pltpu.roll(cells, JL - by, 1), 0.0)
            elif by < 0:
                moved = jnp.where(lanes >= -by, pltpu.roll(cells, -by, 1), 0.0)
            else:
                moved = cells
            shifted_ref[s * 12 + r] = moved

    def one_row(t, carry):
        sums_ref[...] = jnp.zeros((NBASIS, C, JL), F32)
        for k in range(KSUP):
            b = basis_ref[t, k]
            place = (dlon_ref[t, k] + 2) * 12 + dlat_ref[t, k] + 2 + t
            sums_ref[b] = sums_ref[b] + quad_ref[t, k] * shifted_ref[place]
        aggregate = sums_ref[...].astype(BF16).reshape(NBASIS * C, JL)
        rows = pl.ds(t, C, stride=TL)
        after_ref[rows, :] = x_ref[rows, :] + dot(wt_ref[...], aggregate)
        return carry

    lax.fori_loop(0, TL, one_row, 0)


def seam_kernel(
    core_ref,
    dlat_ref,
    dlon_ref,
    basis_ref,
    quad_ref,
    inner_ref,
    far_ref,
    near_ref,
    wt_ref,
    gain_ref,
    after_ref,
    normed_ref,
    scaled_ref,
):
    even = core_ref[0] == 0
    far = far_ref[...].astype(F32)
    near = near_ref[...].astype(F32)
    west = jnp.where(even, far, near)
    east = jnp.where(even, near, far)
    edges = jnp.concatenate([west, east], axis=0).T.astype(BF16)
    row = lax.broadcasted_iota(jnp.int32, (64, 128), 0)
    lane = lax.broadcasted_iota(jnp.int32, (8, 128), 1)
    own = (lane >> 2) & 7
    col = lane & 3
    gather = jnp.zeros((64, 128), F32)
    for k in range(KSUP):
        dlat = jnp.zeros((8, 128), jnp.int32)
        dlon = dlat
        basis = dlat
        quad = jnp.zeros((8, 128), F32)
        for t in range(TL):
            here = own == t
            dlat = jnp.where(here, dlat_ref[t, k], dlat)
            dlon = jnp.where(here, dlon_ref[t, k], dlon)
            basis = jnp.where(here, basis_ref[t, k], basis)
            quad = jnp.where(here, quad_ref[t, k], quad)
        start = 2 * (own + 2 + dlat)
        cell = col + dlon
        source = jnp.where(
            col < 2,
            jnp.where(cell >= 2, 32 + start + cell - 2, -1),
            jnp.where(cell < 2, start + cell, -1),
        )
        source = jnp.where(basis == lane >> 5, source, -1)
        gather = gather + jnp.where(
            row == jnp.concatenate([source] * 8, axis=0), jnp.concatenate([quad] * 8, axis=0), 0.0
        )
    high, low = two_parts(gather)
    sums = dot(edges, high) + dot(edges, low)
    aggregate = jnp.concatenate(
        [sums.astype(BF16)]
        + [pltpu.roll(sums, 128 - 32 * b, 1).astype(BF16) for b in range(1, NBASIS)],
        axis=0,
    )
    seam = dot(wt_ref[...], aggregate)
    lanes = lax.broadcasted_iota(jnp.int32, (C, JL), 1)
    outer = (lanes < 2) | (lanes >= JL - 2)
    for t in range(TL):
        rows = pl.ds(t, C, stride=TL)
        moved = pltpu.roll(seam, (JL - 2 - 4 * t) % JL, 1)
        after = inner_ref[rows, :] + jnp.where(outer, moved, 0.0)
        after_ref[rows, :] = after
        inverse = lax.rsqrt(jnp.sum(after * after, axis=0, keepdims=True) * (1.0 / C) + 1e-6)
        scaled_ref[rows, :] = after * inverse * gain_ref[...]
    normed_ref[...] = scaled_ref[...].astype(BF16)


def chan_block(y, s):
    return s // 2 * 8 + y * 2 + s % 2


def fourier_kernel(recv_ref, lon_ref, lane_ref, out_ref):
    circles = jnp.concatenate(
        [
            jnp.concatenate([recv_ref[chan_block(y, s)] for s in range(8)], axis=1)
            for y in range(4)
        ],
        axis=0,
    )
    found = dot(lon_ref[...], circles, ((1,), (1,)))
    out_ref[...] = dot(found.astype(BF16), lane_ref[...]).astype(BF16)


def spectral_kernel(
    recv_ref, table_ref, filter_ref, out_ref, in_ref, rows_ref, back_ref
):
    first = pl.program_id(0) * STEP

    @pl.when(first == 0)
    def _():
        for j in range(3):
            in_ref[j] = recv_ref[:, 128 * j : 128 * (j + 1)].astype(F32)

    block = lax.broadcasted_iota(jnp.int32, (8, 128), 1) >> 2
    orders = []
    for i in range(STEP):
        parts = []
        for r in range(2):
            for j in range(3):
                near = in_ref[j, pl.ds(r * ORD + first + i, 8, stride=32), :]
                far = in_ref[j, pl.ds(256 + r * ORD + first + i, 8, stride=32), :]
                part = near - far if i % 2 else near + far
                parts.append(pltpu.roll(part, 12 * r + 4 * j, 1) if r + j else part)
        orders.append(parts)
    for yt in range(32):
        place = (block - yt) & 31
        for i in range(STEP):
            tile = orders[i][0]
            for n in range(1, 6):
                tile = jnp.where(place >= n, orders[i][n], tile)
            rows_ref[i, pl.ds(8 * yt, 8), :] = pltpu.roll(tile, 128 - 4 * yt, 1) if yt else tile
    filtered = []
    for i in range(STEP):
        fields = rows_ref[i].astype(BF16)
        spectra = dot(table_ref[0, i], fields)
        filtered.append((spectra * filter_ref[...]).astype(BF16))
    for i in range(STEP):
        rows_ref[i] = dot(table_ref[1, i], filtered[i])
    found = [[None] * 6 for i in range(STEP)]
    for yt in range(32):
        place = (block - yt) & 31
        for i in range(STEP):
            tile = rows_ref[i, pl.ds(8 * yt, 8), :]
            if yt:
                tile = pltpu.roll(tile, 4 * yt, 1)
            for n in range(6):
                found[i][n] = jnp.where(place == n, tile, found[i][n]) if yt else tile
    for i in range(STEP):
        for r in range(2):
            for j in range(3):
                value = found[i][3 * r + j]
                if r + j:
                    value = pltpu.roll(value, 128 - 12 * r - 4 * j, 1)
                back_ref[j, pl.ds(r * ORD + first + i, 8, stride=32), :] = value
                back_ref[j, pl.ds(256 + r * ORD + first + i, 8, stride=32), :] = (
                    -value if i % 2 else value
                )

    @pl.when(first == ORD - STEP)
    def _():
        for j in range(3):
            out_ref[:, 128 * j : 128 * (j + 1)] = back_ref[j].astype(BF16)


def inverse_kernel(recv_ref, lon_ref, lane_ref, out_ref):
    turned = dot(lane_ref[...], recv_ref[...], ((1,), (1,))).astype(BF16)
    for s in range(8):
        lons = pl.ds(128 * s, 128)
        wave = dot(turned, lon_ref[:, lons])
        act = jax.nn.gelu(wave, approximate=True).astype(BF16)
        for y in range(4):
            out_ref[chan_block(y, s)] = act[96 * y : 96 * (y + 1)]


def mix_kernel(act_ref, after_ref, mixt_ref, out_ref, wide_ref):
    wide_ref[...] = act_ref[...].astype(F32)
    for t in range(TL):
        rows = pl.ds(t, C, stride=TL)
        mixed = dot(mixt_ref[...], wide_ref[rows, :].astype(BF16))
        out_ref[rows, :] = after_ref[rows, :] + mixed


def exchanged(blocks, axes):
    return lax.all_to_all(blocks, axes, split_axis=0, concat_axis=0, tiled=True)


def pairs(count, first):
    ends = [(i, (i + 1) % count) for i in range(first, count, 2)]
    return ends + [(j, i) for i, j in ends]


def per_device(
    grid_field,
    disco_dlat,
    disco_dlon,
    disco_basis,
    disco_quad,
    disco_weight,
    norm_gain,
    spectral_filter,
    mix_weight,
):
    forward, backward = longitude_tables()
    lanes = lane_order()
    smem = pl.BlockSpec(memory_space=pltpu.SMEM)
    vmem = pl.BlockSpec(memory_space=pltpu.VMEM)
    x = grid_field.reshape(C * TL, JL)

    lat_count = lax.axis_size(LAT)
    lon_count = lax.axis_size(LON)
    first, last = call(rows_kernel, "rows", 6, (shape((2 * C, JL)), shape((2 * C, JL))))(x)
    up = lax.ppermute(last, LAT, [(i, i + 1) for i in range(lat_count - 1)])
    down = lax.ppermute(first, LAT, [(i + 1, i) for i in range(lat_count - 1)])
    wt, mixt, gain = call(
        weights_kernel,
        "weights",
        10,
        (shape((C, NBASIS * C)), shape((C, C)), shape((C, JL), F32)),
    )(disco_weight.reshape(NBASIS * C, C), mix_weight, norm_gain.reshape(1, C))
    own = lax.dynamic_slice_in_dim(spectral_filter, lax.axis_index(CHAN) * CB, CB, 0)
    own = jnp.concatenate([own, own, jnp.zeros((128 - 2 * CB, LL), F32)], axis=0).T
    up, down, wt, mixt, gain, own = lax.optimization_barrier((up, down, wt, mixt, gain, own))
    core = lax.axis_index("core").astype(jnp.int32).reshape(1)
    far, near = call(
        edges_kernel, "edges", 6, (shape((32, C)), shape((32, C))), in_specs=[smem] + [vmem] * 3
    )(core, x, up, down)
    far = lax.ppermute(far, LON, pairs(lon_count, 1))
    near = lax.ppermute(near, LON, pairs(lon_count, 0))

    place = lax.axis_index(RING).astype(jnp.int32).reshape(1)
    tables = call(
        legendre_kernel,
        "legendre", 57,
        shape((2, ORD, LL, NLAT)),
        in_specs=[smem, smem, vmem, vmem],
        scratch=(pltpu.VMEM((LL * ORD, 128), F32), pltpu.VMEM((LL * ORD, 128), F32)),
    )(place, degree_terms(), order_terms(), latitude_rows())
    tables = pltpu.with_memory_space_constraint(tables, pltpu.HBM)

    inner = call(
        conv_kernel,
        "conv", 24,
        shape((C * TL, JL), F32),
        in_specs=[smem] * 4 + [vmem] * 4,
        scratch=(pltpu.VMEM((60, C, JL), F32), pltpu.VMEM((NBASIS, C, JL), F32)),
    )(disco_dlat, disco_dlon, disco_basis, disco_quad, x, up, down, wt)
    after, normed = call(
        seam_kernel,
        "seam", 12,
        (shape((C * TL, JL), F32), shape((C * TL, JL))),
        in_specs=[smem] * 5 + [vmem] * 5,
        scratch=(pltpu.VMEM((C * TL, JL), F32),),
    )(core, disco_dlat, disco_dlon, disco_basis, disco_quad, inner, far, near, wt, gain)

    portion = exchanged(normed.reshape(32, CB * TL, JL), CHAN)
    fourier = call(fourier_kernel, "fourier", 16, shape((2 * MM, C)))(portion, forward, lanes)
    gathered = exchanged(fourier.reshape(16, 2 * ORD, C), RING)
    whole = pl.BlockSpec((2 * MM, C), lambda m: (0, 0))
    table = pl.BlockSpec((2, STEP, LL, NLAT), lambda m: (0, m, 0, 0))
    synthesis = call(
        spectral_kernel,
        "spectral", 14,
        shape((2 * MM, C)),
        grid=(ORD // STEP,),
        in_specs=[whole, table, pl.BlockSpec((LL, 128), lambda m: (0, 0))],
        out_specs=whole,
        scratch=(
            pltpu.VMEM((3, 2 * MM, 128), F32),
            pltpu.VMEM((STEP, NLAT, 128), F32),
            pltpu.VMEM((3, 2 * MM, 128), F32),
        ),
    )(gathered.reshape(2 * MM, C), tables, own)
    returned = exchanged(synthesis.reshape(16, 2 * ORD, C), RING)
    activated = call(inverse_kernel, "inverse", 16, shape((32, CB * TL, JL)))(
        returned.reshape(2 * MM, C), backward, lanes
    )
    mixed = exchanged(activated, CHAN)
    out = call(
        mix_kernel, "mix", 12, shape((C * TL, JL), F32), scratch=(pltpu.VMEM((C * TL, JL), F32),)
    )(mixed.reshape(C * TL, JL), after, mixt)
    return out.reshape(C, TL, JL)


def solution(mesh):
    torus = Mesh(mesh.devices.reshape(8, 4, 2, 4, 2), ("zl", "y", "zh", "x", "core"))
    placed = (P(None, LAT, LON),) + (P(LAT, None),) * 4 + (P(),) * 4
    return jax.shard_map(
        per_device, mesh=torus, in_specs=placed, out_specs=P(None, LAT, LON), check_vma=False
    )
```
